512 devices in a mesh: seq: 64 (over z, y), head: 8 (over x, core).
Axes of the slice: x: 4, y: 4, z: 16, core: 2. Of those that a mesh axis runs over, the one named last changes fastest.
Arguments:
- hidden_state_input: bfloat16 [16, 8192], P(None, 'seq'), may hold values from -40 to 40
- attention_norm_gain: bfloat16 [8192], P('seq'), may hold values from 0.099609375 to 1.8984375
- query_projection_matrix: bfloat16 [8192, 8192], P('seq', 'head'), may hold values from -0.0625 to 0.0625
- key_projection_matrix: bfloat16 [8192, 1024], P('seq', 'head'), may hold values from -0.0625 to 0.0625
- value_projection_matrix: bfloat16 [8192, 1024], P('seq', 'head'), may hold values from -0.0625 to 0.0625
- output_projection_matrix: bfloat16 [8192, 8192], P('head', 'seq'), may hold values from -0.25 to 0.25
- adapter_down_matrix: bfloat16 [512, 16, 8192], P('head', None, 'seq'), may hold values from -0.0625 to 0.0625
- adapter_up_matrix: bfloat16 [512, 16, 8192], P('seq', None, 'head'), may hold values from -3 to 3
- adapter_choice_index: int32 [16], replicated, may hold values from 0 to 511
- lengths: int32 [16], replicated, may hold values from 4 to 16384
- rotated_key_cache: bfloat16 [16, 16384, 8, 128], P(None, 'seq', 'head'), may hold values from -200 to 200
- cached_value_rows: bfloat16 [16, 16384, 8, 128], P(None, 'seq', 'head'), may hold values from -24 to 24
Outputs:
- output_sum: bfloat16 [16, 8192], P(None, 'seq')
The draws below stay inside these ranges and needn't reach their ends.
Inputs may be any that keep to these rules, and one draw needn't show every extreme that they name: `adapter_choice_index`: index of the adapter that serves each request. The new token stands at position lengths[r]; cache entries at lengths[r] and beyond are not read.
All inputs are finite; a program needn't handle non-finite values.
Results may differ from the reference program's by a relative error of at most 0.025.
Values may be sent and summed in bfloat16 or wider, within the bound.
A program may use at most 64 MiB of HBM per device.

```python
import math
import jax
import jax.numpy as jnp
from jax import lax

MODEL_DIMENSION = 8192
QUERY_HEADS = 64
KVH = 8
HEAD_SIZE = 128
ADAPTER_COUNT = 512
ADAPTER_RANK = 16
REQ = 16
CONTEXT = 16384


def draw_hidden_state_input(key, part):
    key_noise, key_rows, key_cols = jax.random.split(key, 3)
    jitter = jax.random.normal(key_noise, (REQ, MODEL_DIMENSION), jnp.float32)
    lowest = math.log(0.3)
    row_scale = jnp.exp(jax.random.uniform(key_rows, (REQ, 1), jnp.float32, lowest, math.log(3.0)))
    col_scale = jnp.exp(jax.random.uniform(key_cols, (1, MODEL_DIMENSION), jnp.float32, 0.0, math.log(10.0)))
    rising = jnp.exp(jnp.arange(MODEL_DIMENSION, dtype=jnp.float32) * (math.log(3.0) / MODEL_DIMENSION))[None, :]
    return jnp.clip(0.25 * jitter * row_scale * col_scale * rising, -40.0, 40.0).astype(jnp.bfloat16)


def draw_rotated_key_cache(key, part):
    key_base = jax.random.fold_in(key, 0)
    shape_all = (REQ, CONTEXT, KVH, HEAD_SIZE)
    sample = jax.random.normal(key_base, shape_all, jnp.float32)
    return jnp.clip(sample, -200.0, 200.0).astype(jnp.bfloat16)


def plant(drawn, key, low, top_value):
    longest = drawn.shape.index(max(drawn.shape))
    spots = []
    for shift in (0, 1):
        where = [jax.random.randint(jax.random.fold_in(key, axis), (), 0, length) for axis, length in enumerate(drawn.shape)]
        where[longest] = (where[longest] + shift) % drawn.shape[longest]
        spots.append(tuple(where))
    return drawn.at[spots[0]].set(low).at[spots[1]].set(top_value)


def block_scale(rng, dims, shards, smallest, top_value):
    def one(dim, shards_of):
        draws = jax.random.uniform(jax.random.fold_in(jax.random.fold_in(rng, 6), dim), (shards_of,), jnp.float32, smallest / len(shards), top_value / len(shards))
        return jnp.repeat(jnp.exp(draws), dims[dim] // shards_of).reshape((-1,) + (1,) * (len(dims) - dim - 1))

    factor_of = one(*shards[0])
    for cut in shards[1:]:
        factor_of = factor_of * one(*cut)
    return factor_of


def bell_draw(key, shape, width, reach, pieces=(), kind=jnp.bfloat16):
    entries = width * jax.random.normal(key, shape, jnp.float32)
    if pieces:
        entries = entries * block_scale(key, shape, pieces, -0.22, 0.18)
    return jnp.clip(entries, -reach, reach).astype(kind)


def setup_inputs(seed: int = 0) -> dict:
    key_of = jax.random.split(jax.random.key(seed), 13)
    return {
        "hidden_state_input": draw_hidden_state_input(jax.random.fold_in(key_of[12], 71), 0),
        "attention_norm_gain": jnp.clip(1.0 + 0.18 * jax.random.normal(key_of[1], (MODEL_DIMENSION,), jnp.float32), 0.099609375, 1.8984375).astype(jnp.bfloat16),
        "query_projection_matrix": bell_draw(key_of[2], (MODEL_DIMENSION, QUERY_HEADS * HEAD_SIZE), MODEL_DIMENSION ** -0.5, 0.0625, ((0, 64), (1, 8))),
        "key_projection_matrix": bell_draw(key_of[3], (MODEL_DIMENSION, KVH * HEAD_SIZE), MODEL_DIMENSION ** -0.5, 0.0625, ((0, 64), (1, 8))),
        "value_projection_matrix": bell_draw(key_of[4], (MODEL_DIMENSION, KVH * HEAD_SIZE), MODEL_DIMENSION ** -0.5, 0.0625, ((0, 64), (1, 8))),
        "output_projection_matrix": bell_draw(key_of[5], (QUERY_HEADS * HEAD_SIZE, MODEL_DIMENSION), (QUERY_HEADS * HEAD_SIZE // 16) ** -0.5, 0.25, ((0, 8), (1, 64))),
        "adapter_down_matrix": bell_draw(key_of[6], (ADAPTER_COUNT, ADAPTER_RANK, MODEL_DIMENSION), MODEL_DIMENSION ** -0.5, 0.0625, ((0, 8), (2, 64))),
        "adapter_up_matrix": bell_draw(key_of[7], (ADAPTER_COUNT, ADAPTER_RANK, QUERY_HEADS * HEAD_SIZE), (ADAPTER_RANK // 4) ** -0.5, 3.0, ((0, 64), (2, 8))),
        "adapter_choice_index": plant(jax.random.randint(key_of[8], (REQ,), 0, ADAPTER_COUNT), jax.random.fold_in(key_of[8], 1), 0, ADAPTER_COUNT - 1).astype(jnp.int32),
        "lengths": plant(jax.random.randint(key_of[9], (REQ,), 4, CONTEXT + 1), jax.random.fold_in(key_of[9], 1), 4, CONTEXT).astype(jnp.int32),
        "rotated_key_cache": draw_rotated_key_cache(jax.random.fold_in(key_of[12], 71), 0),
        "cached_value_rows": bell_draw(key_of[11], (REQ, CONTEXT, KVH, HEAD_SIZE), 4.0, 24.0, ((1, 64), (2, 8))),
    }


norm_epsilon = 1e-05
adapter_scale_factor = 1.0
rope_base = 500000.0
masked_score = -1e+30

def rotate(vectors, positions):
    half_dim = vectors.shape[-1] // 2
    frequency = jnp.exp(-jnp.arange(half_dim, dtype=jnp.float32) * (jnp.log(jnp.float32(rope_base)) / half_dim))
    angles = positions.astype(jnp.float32)[:, None] * frequency[None, :]
    cosine = jnp.cos(angles)[:, None, :]
    sine_val = jnp.sin(angles)[:, None, :]
    lower_half = vectors[..., :half_dim]
    upper_half = vectors[..., half_dim:]
    return jnp.concatenate([lower_half * cosine - upper_half * sine_val, upper_half * cosine + lower_half * sine_val], axis=-1)

def reference(hidden_state_input, attention_norm_gain, query_projection_matrix, key_projection_matrix, value_projection_matrix, output_projection_matrix, adapter_down_matrix, adapter_up_matrix, adapter_choice_index, lengths, rotated_key_cache, cached_value_rows):
    values32 = hidden_state_input.astype(jnp.float32)
    inverse_factor = lax.rsqrt(lax.optimization_barrier(jnp.mean(values32 * values32, axis=1)) + norm_epsilon)
    scaled = (values32 * attention_norm_gain.astype(jnp.float32)[None, :]).astype(jnp.bfloat16)
    scaled_wide_query = lax.optimization_barrier(scaled).astype(jnp.float32)
    down_map_rows = adapter_down_matrix[adapter_choice_index].astype(jnp.float32)
    reduced_rank_state = (jnp.einsum('by,bey->be', scaled_wide_query, down_map_rows) * inverse_factor[:, None] * adapter_scale_factor).astype(jnp.bfloat16)
    shrunk_wide = lax.optimization_barrier(reduced_rank_state).astype(jnp.float32)
    up_map_rows = adapter_up_matrix[adapter_choice_index].astype(jnp.float32)
    query_full = jnp.dot(scaled, query_projection_matrix, preferred_element_type=jnp.float32) * inverse_factor[:, None] + jnp.einsum('rk,rkc->rc', shrunk_wide, up_map_rows)
    key_new = jnp.dot(scaled, key_projection_matrix, preferred_element_type=jnp.float32) * inverse_factor[:, None]
    value_new = jnp.dot(scaled, value_projection_matrix, preferred_element_type=jnp.float32) * inverse_factor[:, None]
    query_rot = rotate(query_full.reshape(REQ, QUERY_HEADS, HEAD_SIZE), lengths).astype(jnp.bfloat16)
    key_rot = rotate(key_new.reshape(REQ, KVH, HEAD_SIZE), lengths).astype(jnp.bfloat16)
    value_own = value_new.reshape(REQ, KVH, HEAD_SIZE).astype(jnp.bfloat16)
    grouped = query_rot.reshape(REQ, KVH, QUERY_HEADS // KVH, HEAD_SIZE)
    score_scale = HEAD_SIZE ** (-0.5)

    def one_request(request_items):
        query_one, key_rows, value_rows, length, own_key, own_value = request_items
        query_wide = query_one.astype(jnp.float32)
        scores = jnp.einsum('hgd,jhd->hgj', query_wide, key_rows.astype(jnp.float32)) * score_scale
        valid_mask = jnp.arange(CONTEXT) < length
        scores = jnp.where(valid_mask[None, None, :], scores, masked_score)
        own_score = jnp.einsum('hgd,hd->hg', query_wide, own_key.astype(jnp.float32)) * score_scale
        peak = jnp.maximum(lax.optimization_barrier(jnp.max(scores, axis=-1)), own_score)
        weights = jnp.where(valid_mask[None, None, :], jnp.exp(scores - peak[..., None]), 0.0)
        own_weight = jnp.exp(own_score - peak)
        denominator = lax.optimization_barrier(jnp.sum(weights, axis=-1)) + own_weight
        probs = lax.optimization_barrier(weights.astype(jnp.bfloat16)).astype(jnp.float32)
        summed = jnp.einsum('hgj,jhd->hgd', probs, value_rows.astype(jnp.float32))
        summed = summed + own_weight[..., None] * own_value.astype(jnp.float32)[:, None, :]
        return (summed / denominator[..., None]).astype(jnp.bfloat16)
    attended = lax.map(one_request, (grouped, rotated_key_cache, cached_value_rows, lengths, key_rot, value_own))
    attended = attended.reshape(REQ, QUERY_HEADS * HEAD_SIZE)
    return jnp.dot(attended, output_projection_matrix, preferred_element_type=jnp.float32).astype(jnp.bfloat16)
```

```python
import jax
import jax.numpy as jnp
from jax import lax
from jax.experimental import pallas as pl
from jax.experimental.pallas import tpu as pltpu
from jax.sharding import PartitionSpec as P

MESH = pl.DeviceIdType.MESH
F32 = jnp.float32
BF16 = jnp.bfloat16

norm_epsilon = 1e-05
rope_base = 500000.0
masked_score = -1e30

NY, NZ, NH = 4, 16, 8
PLANE = [(dy, dh) for dy in range(NY) for dh in range(NH) if (dy, dh) != (0, 0)]
COLUMN = list(range(1, NZ))
WINDOW = [(dy, dz) for dz in (2, -1, 1, 0) for dy in (2, 1, 3, 0) if (dy, dz) != (0, 0)]
QUARTER = [8, 4, 12]
HEADS = list(range(1, NH))
STAGES = 11


def kernel(
    hid_h, gain_h, wq_h, wk_h, wv_h, wo_h, down_h, up_h, choice, lengths, kc_h, vc_h,
    out,
    hid, gain, wq, wk, wv, wo, down, up, kc, vc,
    t1a, t1b, rsb_src, rsb, z2b, rse_src, rse, z2e, agq, rso_src, rso, z2o, ago, hbuf,
    load_sem, send_sem, recv_sem,
):
    seq = lax.axis_index("seq")
    head = lax.axis_index("head")
    y = lax.rem(seq, NY)
    z = lax.div(seq, NY)
    mine = y * 4 + lax.rem(z, 4)

    def at(dy, dz, dh):
        yy = lax.rem(y + (dy + NY) % NY, NY)
        zz = lax.rem(z + (dz + NZ) % NZ, NZ)
        return (zz * NY + yy, lax.rem(head + (dh + NH) % NH, NH))

    barrier = pltpu.get_barrier_semaphore()
    greeted = [(0, dz, 0) for dz in COLUMN]
    greeted += [(-dy, -dz, 0) for dy, dz in WINDOW if dy and dz]
    greeted += [(dy, 0, dh) for dy, dh in PLANE]
    for dy, dz, dh in greeted:
        pl.semaphore_signal(barrier, inc=1, device_id=at(dy, dz, dh), device_id_type=MESH)

    loads = [
        pltpu.make_async_copy(src, dst, load_sem.at[k])
        for k, (src, dst) in enumerate(
            [(hid_h, hid), (gain_h, gain), (down_h, down), (wq_h, wq), (wk_h, wk), (wv_h, wv),
             (up_h, up), (kc_h, kc), (vc_h, vc), (wo_h, wo)]
        )
    ]
    for c in loads:
        c.start()

    def send(stage, src, dst, where):
        pltpu.make_async_remote_copy(
            src_ref=src, dst_ref=dst, send_sem=send_sem.at[stage], recv_sem=recv_sem.at[stage],
            device_id=at(*where), device_id_type=MESH,
        ).start()

    def bundle(stage, view):
        return pltpu.make_async_remote_copy(
            src_ref=view, dst_ref=view, send_sem=send_sem.at[stage], recv_sem=recv_sem.at[stage],
            device_id=at(0, 1, 0), device_id_type=MESH,
        )

    rows = lax.broadcasted_iota(jnp.int32, (16, 128), 0)
    lane = lax.broadcasted_iota(jnp.int32, (16, 128), 1)
    group = lane // 16
    rows8 = lax.rem(rows, 8)
    lane8 = lax.broadcasted_iota(jnp.int32, (8, 128), 1)
    chosen = jnp.zeros((16, 128), jnp.int32)
    for r in range(16):
        chosen = jnp.where(rows == r, choice[r], chosen)

    for c in loads[:3]:
        c.wait()
    values = hid[...].astype(F32)
    scaled = (values * gain[...].astype(F32)).astype(BF16)
    every = lax.dot_general(
        scaled, down[...], (((1,), (1,)), ((), ())), preferred_element_type=F32
    )
    fold = jnp.zeros((16, 128), F32)
    for j in range(8):
        fold += jnp.where(
            chosen == head * 64 + j * 8 + group, every[:, j * 128 : (j + 1) * 128], 0.0
        )
    for shift in (64, 32, 16):
        fold += pltpu.roll(fold, shift, 1)
    diagonal = jnp.where(group == rows8, fold, 0.0)
    square = jnp.sum(values * values, axis=1, keepdims=True)
    t1a[0, 0:1, :] = jnp.sum(diagonal[0:8], axis=0, keepdims=True)
    t1a[0, 1:2, :] = jnp.sum(diagonal[8:16], axis=0, keepdims=True)
    t1a[0, 2:3, :] = jnp.sum(jnp.where(lane == rows, square, 0.0), axis=0, keepdims=True)
    t1a[0, 3:4, :] = jnp.zeros((1, 128), F32)

    pl.semaphore_wait(barrier, len(greeted))
    for k, (dy, dh) in enumerate(PLANE):
        send(0, t1a.at[0], t1a.at[k + 1], (dy, 0, dh))

    for c in loads[3:6]:
        c.wait()
    query_part = jnp.dot(scaled, wq[...], preferred_element_type=F32)
    key_part = jnp.dot(scaled, wk[...], preferred_element_type=F32)
    value_part = jnp.dot(scaled, wv[...], preferred_element_type=F32)
    for j in range(8):
        rsb_src[pl.ds(j, 16, stride=16), :] = query_part[:, j * 128 : (j + 1) * 128]
    rsb_src[pl.ds(8, 16, stride=16), :] = key_part
    rsb_src[pl.ds(9, 16, stride=16), :] = value_part
    for j in range(10, 16):
        rsb_src[pl.ds(j, 16, stride=16), :] = jnp.zeros((16, 128), F32)

    def row_of(dy, dz):
        return lax.rem(y + dy, 4) * 4 + lax.rem(lax.rem(z, 4) + dz + 4, 4)

    def rows_at(r, n):
        return pl.ds(pl.multiple_of(r * n, n), n)

    for k, (dy, dz) in enumerate(WINDOW):
        send(2, rsb_src.at[rows_at(row_of(dy, dz), 16)], rsb.at[k], (dy, dz, 0))

    bundle(0, t1a.at[1:32]).wait_recv()
    t1b[0] = jnp.sum(t1a[...], axis=0)
    for k, dz in enumerate(COLUMN):
        send(1, t1b.at[0], t1b.at[k + 1], (0, dz, 0))

    bundle(2, rsb).wait_recv()
    base = rsb_src[rows_at(mine, 16), :]
    for k in range(15):
        base += rsb[k]
    z2b[0] = base
    for k, dz in enumerate(QUARTER):
        send(3, z2b.at[0], z2b.at[k + 1], (0, dz, 0))

    bundle(1, t1b.at[1:16]).wait_recv()
    whole = jnp.sum(t1b[...], axis=0)
    spread = jnp.concatenate(
        [jnp.broadcast_to(whole[0:1], (8, 128)), jnp.broadcast_to(whole[1:2], (8, 128))], axis=0
    )
    spread = jnp.where(group == rows8, spread, 0.0)
    for shift in (64, 32, 16):
        spread += pltpu.roll(spread, shift, 1)
    squares = jnp.sum(
        jnp.where(lane == rows, jnp.broadcast_to(whole[2:3], (16, 128)), 0.0),
        axis=1,
        keepdims=True,
    )
    inverse = lax.rsqrt(squares * (1.0 / (NH * 8192.0)) + norm_epsilon)
    shrunk = (spread * inverse).astype(BF16).astype(F32)
    placed = jnp.where(chosen == seq * 8 + group, shrunk, 0.0).astype(BF16)
    loads[6].wait()
    expand = jnp.dot(placed, up[...], preferred_element_type=F32)
    for j in range(8):
        rse_src[pl.ds(j, 16, stride=8), :] = expand[:, j * 128 : (j + 1) * 128]
    for k, (dy, dz) in enumerate(WINDOW):
        send(4, rse_src.at[rows_at(row_of(dy, dz), 8)], rse.at[k], (dy, dz, 0))

    inverse_mine = jnp.sum(jnp.where(rows == mine, inverse, 0.0), axis=0, keepdims=True)
    half = lax.rem(lane8, 64).astype(F32)
    frequency = jnp.exp(-half * (jnp.log(jnp.full((8, 128), rope_base, F32)) / 64.0))
    angle = lengths[mine].astype(F32) * frequency
    cosine = jnp.cos(angle)
    sine = jnp.where(lane8 < 64, -jnp.sin(angle), jnp.sin(angle))

    bundle(3, z2b.at[1:4]).wait_recv()
    base = (z2b[0] + z2b[1]) + (z2b[2] + z2b[3])
    base = base * inverse_mine
    bundle(4, rse).wait_recv()
    grown = rse_src[rows_at(mine, 8), :]
    for k in range(15):
        grown += rse[k]
    z2e[0] = grown
    for k, dz in enumerate(QUARTER):
        send(5, z2e.at[0], z2e.at[k + 1], (0, dz, 0))

    def rotated(x):
        return (x * cosine + pltpu.roll(x, 64, 1) * sine).astype(BF16)

    key_rot = rotated(jnp.broadcast_to(base[8:9], (8, 128))).astype(F32)
    value_own = jnp.broadcast_to(base[9:10], (8, 128)).astype(BF16).astype(F32)
    bundle(5, z2e.at[1:4]).wait_recv()
    query = base[0:8] + ((z2e[0] + z2e[1]) + (z2e[2] + z2e[3]))
    query_rot = rotated(query)
    agq[mine] = query_rot
    for dy, dz in WINDOW:
        send(6, agq.at[mine], agq.at[mine], (dy, dz, 0))
    scale = 128.0**-0.5
    own_score = jnp.sum(query_rot.astype(F32) * key_rot, axis=1, keepdims=True) * scale

    loads[7].wait()
    loads[8].wait()
    bundle(6, agq.at[0:15]).wait_recv()
    position = lax.broadcasted_iota(jnp.int32, (8, 256), 1) + seq * 256
    for r in range(16):
        scores = (
            lax.dot_general(agq[r], kc[r], (((1,), (1,)), ((), ())), preferred_element_type=F32)
            * scale
        )
        valid = position < lengths[r]
        scores = jnp.where(valid, scores, masked_score)
        top = jnp.max(scores, axis=1, keepdims=True)
        weights = jnp.where(valid, jnp.exp(scores - top), 0.0)
        total = jnp.sum(weights, axis=1, keepdims=True)
        rso_src[r, 0:8, :] = jnp.dot(weights.astype(BF16), vc[r], preferred_element_type=F32)
        rso_src[r, 8:16, :] = jnp.where(lane8 < 64, top, total)
    for k, (dy, dz) in enumerate(WINDOW):
        send(7, rso_src.at[row_of(dy, dz)], rso.at[k], (dy, dz, 0))

    def merged(parts):
        tops, totals, outs = [], [], []
        for part in parts:
            stat = part[8:16]
            swapped = pltpu.roll(stat, 64, 1)
            tops.append(jnp.where(lane8 < 64, stat, swapped))
            totals.append(jnp.where(lane8 < 64, swapped, stat))
            outs.append(part[0:8])
        top = tops[0]
        for t in tops[1:]:
            top = jnp.maximum(top, t)
        total = jnp.zeros((8, 128), F32)
        result = jnp.zeros((8, 128), F32)
        for t, s, o in zip(tops, totals, outs):
            factor = jnp.exp(t - top)
            total += s * factor
            result += o * factor
        return top, total, result

    bundle(7, rso).wait_recv()
    top, total, result = merged([rso_src[mine]] + [rso[k] for k in range(15)])
    z2o[0, 0:8, :] = result
    z2o[0, 8:16, :] = jnp.where(lane8 < 64, top, total)
    for k, dz in enumerate(QUARTER):
        send(8, z2o.at[0], z2o.at[k + 1], (0, dz, 0))
    bundle(8, z2o.at[1:4]).wait_recv()
    top, total, result = merged([z2o[k] for k in range(4)])
    peak = jnp.maximum(top, own_score)
    factor = jnp.exp(top - peak)
    own_weight = jnp.exp(own_score - peak)
    attended = (result * factor + own_weight * value_own) / (total * factor + own_weight)
    ago[rows_at(mine, 8), :] = attended.astype(BF16).astype(F32)
    for dy, dz in WINDOW:
        send(9, ago.at[rows_at(mine, 8)], ago.at[rows_at(mine, 8)], (dy, dz, 0))

    loads[9].wait()
    bundle(9, ago.at[0:120]).wait_recv()
    projected = jnp.zeros((16, 128), F32)
    for j in range(8):
        projected += jnp.dot(
            ago[pl.ds(j, 16, stride=8), :].astype(BF16),
            wo[j * 128 : (j + 1) * 128, :],
            preferred_element_type=F32,
        )
    hbuf[0] = projected
    for k, dh in enumerate(HEADS):
        send(10, hbuf.at[0], hbuf.at[k + 1], (0, 0, dh))
    bundle(10, hbuf.at[1:8]).wait_recv()
    out[...] = jnp.sum(hbuf[...], axis=0).astype(BF16)

    for stage, view in enumerate(
        [t1a.at[1:32], t1b.at[1:16], rsb, z2b.at[1:4], rse, z2e.at[1:4], agq.at[0:15], rso,
         z2o.at[1:4], ago.at[0:120], hbuf.at[1:8]]
    ):
        bundle(stage, view).wait_send()


def body(hid, gain, wq, wk, wv, wo, down, up, choice, lengths, kc, vc):
    anywhere = pl.BlockSpec(memory_space=pl.ANY)
    scalars = pl.BlockSpec(memory_space=pltpu.SMEM)
    return pl.pallas_call(
        kernel,
        out_shape=jax.ShapeDtypeStruct((16, 128), BF16),
        in_specs=[anywhere] * 8 + [scalars] * 2 + [anywhere] * 2,
        out_specs=pl.BlockSpec(memory_space=pltpu.VMEM),
        scratch_shapes=[
            pltpu.VMEM((16, 128), BF16),
            pltpu.VMEM((1, 128), BF16),
            pltpu.VMEM((128, 1024), BF16),
            pltpu.VMEM((128, 128), BF16),
            pltpu.VMEM((128, 128), BF16),
            pltpu.VMEM((1024, 128), BF16),
            pltpu.VMEM((1024, 128), BF16),
            pltpu.VMEM((128, 1024), BF16),
            pltpu.VMEM((16, 256, 128), BF16),
            pltpu.VMEM((16, 256, 128), BF16),
            pltpu.VMEM((32, 4, 128), F32),
            pltpu.VMEM((16, 4, 128), F32),
            pltpu.VMEM((256, 128), F32),
            pltpu.VMEM((15, 16, 128), F32),
            pltpu.VMEM((4, 16, 128), F32),
            pltpu.VMEM((128, 128), F32),
            pltpu.VMEM((15, 8, 128), F32),
            pltpu.VMEM((4, 8, 128), F32),
            pltpu.VMEM((16, 8, 128), BF16),
            pltpu.VMEM((16, 16, 128), F32),
            pltpu.VMEM((15, 16, 128), F32),
            pltpu.VMEM((4, 16, 128), F32),
            pltpu.VMEM((128, 128), F32),
            pltpu.VMEM((8, 16, 128), F32),
            pltpu.SemaphoreType.DMA((10,)),
            pltpu.SemaphoreType.DMA((STAGES,)),
            pltpu.SemaphoreType.DMA((STAGES,)),
        ],
        compiler_params=pltpu.CompilerParams(collective_id=0, has_side_effects=True),
    )(
        hid, gain.reshape(1, 128), wq, wk, wv, wo, down.reshape(1024, 128), up.reshape(128, 1024),
        choice, lengths, kc.reshape(16, 256, 128), vc.reshape(16, 256, 128),
    )


def solution(mesh):
    placed = (
        P(None, "seq"),
        P("seq"),
        P("seq", "head"),
        P("seq", "head"),
        P("seq", "head"),
        P("head", "seq"),
        P("head", None, "seq"),
        P("seq", None, "head"),
        P(),
        P(),
        P(None, "seq", "head", None),
        P(None, "seq", "head", None),
    )
    return jax.shard_map(
        body, mesh=mesh, in_specs=placed, out_specs=P(None, "seq"), check_vma=False
    )
```

```python
import jax
import jax.numpy as jnp
from jax import lax
from jax.experimental import pallas as pl
from jax.experimental.pallas import tpu as pltpu
from jax.sharding import PartitionSpec as P

MESH = pl.DeviceIdType.MESH
F32 = jnp.float32
BF16 = jnp.bfloat16

norm_epsilon = 1e-05
rope_base = 500000.0
masked_score = -1e30

NY, NZ, NH = 4, 16, 8
PLANE = [(dy, dh) for dy in range(NY) for dh in range(NH) if (dy, dh) != (0, 0)]
COLUMN = list(range(1, NZ))
WINDOW = [(dy, dz) for dz in (2, -1, 1, 0) for dy in (2, 1, 3, 0) if (dy, dz) != (0, 0)]
QUARTER = [8, 4, 12]
HEADS = list(range(1, NH))
NEAR = [1, -1, 2, -2, 3, -3, 4, -4]
STAGES = 11


def kernel(
    hid_h, gain_h, wq_h, wk_h, wv_h, wo_h, down_h, up_h, choice_h, lengths_h, kc_h, vc_h,
    out,
    hid, gain, wq, wk, wv, wo, down, up, kc, vc, choice, lengths,
    t1a, t1b, flat, rsb_src, rsb, z2b, rse_src, rse, z2e, agq, rso_src, rso, z2o, ago, hbuf,
    load_sem, send_sem, recv_sem, vouch,
):
    seq = lax.axis_index("seq")
    head = lax.axis_index("head")
    y = lax.rem(seq, NY)
    z = lax.div(seq, NY)
    mine = y * 4 + lax.rem(z, 4)

    def at(dy, dz, dh):
        yy = lax.rem(y + (dy + NY) % NY, NY)
        zz = lax.rem(z + (dz + NZ) % NZ, NZ)
        return (zz * NY + yy, lax.rem(head + (dh + NH) % NH, NH))

    barrier = pltpu.get_barrier_semaphore()
    greeted = [(0, dz, 0) for dz in NEAR]
    greeted += [(-dy, -dz, 0) for dy, dz in WINDOW if dy and dz]
    greeted += [(dy, 0, dh) for dy, dh in PLANE]
    for dy, dz, dh in greeted:
        pl.semaphore_signal(barrier, inc=1, device_id=at(dy, dz, dh), device_id_type=MESH)

    loads = [
        pltpu.make_async_copy(src, dst, load_sem.at[k])
        for k, (src, dst) in enumerate(
            [(hid_h, hid), (gain_h, gain), (down_h, down), (wq_h, wq), (wk_h, wk), (wv_h, wv),
             (up_h, up), (kc_h, kc), (vc_h, vc), (wo_h, wo), (choice_h, choice),
             (lengths_h, lengths)]
        )
    ]
    for c in loads:
        c.start()

    def send(stage, src, dst, where):
        pltpu.make_async_remote_copy(
            src_ref=src, dst_ref=dst, send_sem=send_sem.at[stage], recv_sem=recv_sem.at[stage],
            device_id=at(*where), device_id_type=MESH,
        ).start()

    def bundle(stage, view):
        return pltpu.make_async_remote_copy(
            src_ref=view, dst_ref=view, send_sem=send_sem.at[stage], recv_sem=recv_sem.at[stage],
            device_id=at(0, 1, 0), device_id_type=MESH,
        )

    rows = lax.broadcasted_iota(jnp.int32, (16, 128), 0)
    lane = lax.broadcasted_iota(jnp.int32, (16, 128), 1)
    group = lane // 16
    rows8 = lax.rem(rows, 8)
    lane8 = lax.broadcasted_iota(jnp.int32, (8, 128), 1)
    loads[10].wait()
    chosen = jnp.zeros((16, 128), jnp.int32)
    for r in range(16):
        chosen = jnp.where(rows == r, choice[r], chosen)

    for c in loads[:3]:
        c.wait()
    values = hid[...].astype(F32)
    scaled = (values * gain[...].astype(F32)).astype(BF16)
    every = lax.dot_general(
        scaled, down[...], (((1,), (1,)), ((), ())), preferred_element_type=F32
    )
    fold = jnp.zeros((16, 128), F32)
    for j in range(8):
        fold += jnp.where(
            chosen == head * 64 + j * 8 + group, every[:, j * 128 : (j + 1) * 128], 0.0
        )
    for shift in (64, 32, 16):
        fold += pltpu.roll(fold, shift, 1)
    diagonal = jnp.where(group == rows8, fold, 0.0)
    square = jnp.sum(values * values, axis=1, keepdims=True)
    t1a[0, 0:1, :] = jnp.sum(diagonal[0:8], axis=0, keepdims=True)
    t1a[0, 1:2, :] = jnp.sum(diagonal[8:16], axis=0, keepdims=True)

    pl.semaphore_wait(barrier, len(greeted))
    for k, (dy, dh) in enumerate(PLANE):
        send(0, t1a.at[0], t1a.at[k + 1], (dy, 0, dh))
    for dz in (4, -4):
        pl.semaphore_signal(vouch, inc=1, device_id=at(0, dz, 0), device_id_type=MESH)

    for c in loads[3:6]:
        c.wait()
    query_part = jnp.dot(scaled, wq[...], preferred_element_type=F32)
    key_part = jnp.dot(scaled, wk[...], preferred_element_type=F32)
    value_part = jnp.dot(scaled, wv[...], preferred_element_type=F32)
    for j in range(8):
        flat[pl.ds(j, 16, stride=16), :] = query_part[:, j * 128 : (j + 1) * 128]
    flat[pl.ds(8, 16, stride=16), :] = key_part
    flat[pl.ds(9, 16, stride=16), :] = value_part
    flat[pl.ds(10, 16, stride=16), :] = jnp.broadcast_to(square, (16, 128))
    for j in range(11, 16):
        flat[pl.ds(j, 16, stride=16), :] = jnp.zeros((16, 128), F32)
    rsb_src[...] = flat[...].reshape(16, 16, 128).astype(BF16)

    def row_of(dy, dz):
        return lax.rem(y + dy, 4) * 4 + lax.rem(lax.rem(z, 4) + dz + 4, 4)

    for k, (dy, dz) in enumerate(WINDOW):
        send(2, rsb_src.at[row_of(dy, dz)], rsb.at[k], (dy, dz, 0))

    bundle(0, t1a.at[1:32]).wait_recv()
    t1b[0] = jnp.sum(t1a[...], axis=0)
    pl.semaphore_wait(vouch, 2)
    for k, dz in enumerate(COLUMN):
        send(1, t1b.at[0], t1b.at[k + 1], (0, dz, 0))

    bundle(2, rsb).wait_recv()
    base = rsb_src[mine].astype(F32)
    for k in range(15):
        base += rsb[k].astype(F32)
    z2b[0] = base.astype(BF16)
    for k, dz in enumerate(QUARTER):
        send(3, z2b.at[0], z2b.at[k + 1], (0, dz, 0))

    loads[11].wait()
    half = lax.rem(lane8, 64).astype(F32)
    frequency = jnp.exp(-half * (jnp.log(jnp.full((8, 128), rope_base, F32)) / 64.0))
    angle = lengths[mine].astype(F32) * frequency
    cosine = jnp.cos(angle)
    sine = jnp.sin(angle)
    sine = jnp.where(lane8 < 64, -sine, sine)

    loads[6].wait()
    bundle(1, t1b.at[1:16]).wait_recv()
    whole = jnp.sum(t1b[...], axis=0)
    spread = jnp.concatenate(
        [jnp.broadcast_to(whole[0:1], (8, 128)), jnp.broadcast_to(whole[1:2], (8, 128))], axis=0
    )
    spread = jnp.where(group == rows8, spread, 0.0)
    for shift in (64, 32, 16):
        spread += pltpu.roll(spread, shift, 1)
    placed = jnp.where(chosen == seq * 8 + group, spread, 0.0).astype(BF16)
    expand = jnp.dot(placed, up[...], preferred_element_type=F32)
    for j in range(8):
        flat[pl.ds(j, 16, stride=8), :] = expand[:, j * 128 : (j + 1) * 128]
    rse_src[...] = flat[0:128, :].reshape(16, 8, 128).astype(BF16)
    for k, (dy, dz) in enumerate(WINDOW):
        send(4, rse_src.at[row_of(dy, dz)], rse.at[k], (dy, dz, 0))

    bundle(3, z2b.at[1:4]).wait_recv()
    base = z2b[0].astype(F32)
    for k in range(1, 4):
        base += z2b[k].astype(F32)
    inverse = lax.rsqrt(base[10:11] * (1.0 / 8192.0) + norm_epsilon)
    bundle(4, rse).wait_recv()
    grown = rse_src[mine].astype(F32)
    for k in range(15):
        grown += rse[k].astype(F32)
    z2e[0] = grown.astype(BF16)
    for k, dz in enumerate(QUARTER):
        send(5, z2e.at[0], z2e.at[k + 1], (0, dz, 0))

    def rotated(x):
        return (x * cosine + pltpu.roll(x, 64, 1) * sine).astype(BF16)

    key_rot = rotated(jnp.broadcast_to(base[8:9] * inverse, (8, 128))).astype(F32)
    value_own = jnp.broadcast_to(base[9:10] * inverse, (8, 128)).astype(BF16).astype(F32)
    bundle(5, z2e.at[1:4]).wait_recv()
    query = base[0:8]
    for k in range(4):
        query += z2e[k].astype(F32)
    query_rot = rotated(query * inverse)
    agq[mine] = query_rot
    for dy, dz in WINDOW:
        send(6, agq.at[mine], agq.at[mine], (dy, dz, 0))
    scale = 128.0**-0.5
    own_score = jnp.sum(query_rot.astype(F32) * key_rot, axis=1, keepdims=True) * scale

    def packed(high, low, total, result):
        stat = jnp.where(lane8 < 32, high, jnp.where(lane8 < 64, low, total))
        return jnp.concatenate([result, stat], axis=0).astype(BF16)

    def merged(parts):
        parts = [part.astype(F32) for part in parts]
        stats = [part[8:16] for part in parts]
        tops = [
            jnp.broadcast_to(stat[:, 0:1] + stat[:, 32:33], (8, 128)) for stat in stats
        ]
        totals = [jnp.broadcast_to(stat[:, 64:65], (8, 128)) for stat in stats]
        top = tops[0]
        for t in tops[1:]:
            top = jnp.maximum(top, t)
        high = top.astype(BF16).astype(F32)
        low = (top - high).astype(BF16).astype(F32)
        total = jnp.zeros((8, 128), F32)
        result = jnp.zeros((8, 128), F32)
        for t, s, part in zip(tops, totals, parts):
            factor = jnp.exp(t - (high + low))
            total += s * factor
            result += part[0:8] * factor
        return high, low, total, result

    loads[7].wait()
    loads[8].wait()
    bundle(6, agq.at[0:15]).wait_recv()
    position = lax.broadcasted_iota(jnp.int32, (8, 256), 1) + seq * 256
    each = range(16)
    scores = [
        lax.dot_general(agq[r], kc[r], (((1,), (1,)), ((), ())), preferred_element_type=F32)
        * scale
        for r in each
    ]
    valid = [position < lengths[r] for r in each]
    scores = [jnp.where(valid[r], scores[r], masked_score) for r in each]
    tops = [jnp.max(scores[r], axis=1, keepdims=True) for r in each]
    highs = [top.astype(BF16).astype(F32) for top in tops]
    lows = [(top - high).astype(BF16).astype(F32) for top, high in zip(tops, highs)]
    weights = [
        jnp.where(valid[r], jnp.exp(scores[r] - (highs[r] + lows[r])), 0.0) for r in each
    ]
    totals = [jnp.sum(weights[r], axis=1, keepdims=True) for r in each]
    results = [
        jnp.dot(weights[r].astype(BF16), vc[r], preferred_element_type=F32) for r in each
    ]
    for r in each:
        rso_src[r] = packed(highs[r], lows[r], totals[r], results[r])
    for k, (dy, dz) in enumerate(WINDOW):
        send(7, rso_src.at[row_of(dy, dz)], rso.at[k], (dy, dz, 0))

    bundle(7, rso).wait_recv()
    z2o[0] = packed(*merged([rso_src[mine]] + [rso[k] for k in range(15)]))
    for k, dz in enumerate(QUARTER):
        send(8, z2o.at[0], z2o.at[k + 1], (0, dz, 0))
    bundle(8, z2o.at[1:4]).wait_recv()
    high, low, total, result = merged([z2o[k] for k in range(4)])
    top = high + low
    peak = jnp.maximum(top, own_score)
    factor = jnp.exp(top - peak)
    own_weight = jnp.exp(own_score - peak)
    attended = (result * factor + own_weight * value_own) / (total * factor + own_weight)
    ago[mine] = attended.astype(BF16)
    for dy, dz in WINDOW:
        send(9, ago.at[mine], ago.at[mine], (dy, dz, 0))

    loads[9].wait()
    bundle(9, ago.at[0:15]).wait_recv()
    flat[0:128, :] = ago[...].astype(F32).reshape(128, 128)
    projected = jnp.zeros((16, 128), F32)
    for j in range(8):
        projected += jnp.dot(
            flat[pl.ds(j, 16, stride=8), :].astype(BF16),
            wo[j * 128 : (j + 1) * 128, :],
            preferred_element_type=F32,
        )
    hbuf[0] = projected.astype(BF16)
    for k, dh in enumerate(HEADS):
        send(10, hbuf.at[0], hbuf.at[k + 1], (0, 0, dh))
    bundle(10, hbuf.at[1:8]).wait_recv()
    out[...] = jnp.sum(hbuf[...].astype(F32), axis=0).astype(BF16)

    for stage, view in enumerate(
        [t1a.at[1:32], t1b.at[1:16], rsb, z2b.at[1:4], rse, z2e.at[1:4], agq.at[0:15], rso,
         z2o.at[1:4], ago.at[0:15], hbuf.at[1:8]]
    ):
        bundle(stage, view).wait_send()


def body(hid, gain, wq, wk, wv, wo, down, up, choice, lengths, kc, vc):
    anywhere = pl.BlockSpec(memory_space=pl.ANY)
    return pl.pallas_call(
        kernel,
        out_shape=pltpu.VMEM((16, 128), BF16),
        in_specs=[anywhere] * 12,
        out_specs=pl.BlockSpec(memory_space=pltpu.VMEM),
        scratch_shapes=[
            pltpu.VMEM((16, 128), BF16),
            pltpu.VMEM((1, 128), BF16),
            pltpu.VMEM((128, 1024), BF16),
            pltpu.VMEM((128, 128), BF16),
            pltpu.VMEM((128, 128), BF16),
            pltpu.VMEM((1024, 128), BF16),
            pltpu.VMEM((1024, 128), BF16),
            pltpu.VMEM((128, 1024), BF16),
            pltpu.VMEM((16, 256, 128), BF16),
            pltpu.VMEM((16, 256, 128), BF16),
            pltpu.SMEM((16,), jnp.int32),
            pltpu.SMEM((16,), jnp.int32),
            pltpu.VMEM((32, 2, 128), F32),
            pltpu.VMEM((16, 2, 128), F32),
            pltpu.VMEM((256, 128), F32),
            pltpu.VMEM((16, 16, 128), BF16),
            pltpu.VMEM((15, 16, 128), BF16),
            pltpu.VMEM((4, 16, 128), BF16),
            pltpu.VMEM((16, 8, 128), BF16),
            pltpu.VMEM((15, 8, 128), BF16),
            pltpu.VMEM((4, 8, 128), BF16),
            pltpu.VMEM((16, 8, 128), BF16),
            pltpu.VMEM((16, 16, 128), BF16),
            pltpu.VMEM((15, 16, 128), BF16),
            pltpu.VMEM((4, 16, 128), BF16),
            pltpu.VMEM((16, 8, 128), BF16),
            pltpu.VMEM((8, 16, 128), BF16),
            pltpu.SemaphoreType.DMA((12,)),
            pltpu.SemaphoreType.DMA((STAGES,)),
            pltpu.SemaphoreType.DMA((STAGES,)),
            pltpu.SemaphoreType.REGULAR,
        ],
        compiler_params=pltpu.CompilerParams(collective_id=0, has_side_effects=True),
    )(
        hid, gain.reshape(1, 128), wq, wk, wv, wo, down.reshape(1024, 128), up.reshape(128, 1024),
        choice, lengths, kc.reshape(16, 256, 128), vc.reshape(16, 256, 128),
    )


def solution(mesh):
    placed = (
        P(None, "seq"),
        P("seq"),
        P("seq", "head"),
        P("seq", "head"),
        P("seq", "head"),
        P("head", "seq"),
        P("head", None, "seq"),
        P("seq", None, "head"),
        P(),
        P(),
        P(None, "seq", "head", None),
        P(None, "seq", "head", None),
    )
    return jax.shard_map(
        body, mesh=mesh, in_specs=placed, out_specs=P(None, "seq"), check_vma=False
    )
```

```python
import jax
import jax.numpy as jnp
from jax import lax
from jax.experimental import pallas as pl
from jax.experimental.pallas import tpu as pltpu
from jax.sharding import PartitionSpec as P

MESH = pl.DeviceIdType.MESH
F32 = jnp.float32
BF16 = jnp.bfloat16

norm_epsilon = 1e-05
rope_base = 500000.0
masked_score = -1e30

NY, NZ, NH = 4, 16, 8
PLANE = [(dy, dh) for dy in range(NY) for dh in range(NH) if (dy, dh) != (0, 0)]
COLUMN = list(range(1, NZ))
WINDOW = [(dy, dz) for dy in (2, 1, 3) for dz in (2 if dy == 2 else -2, 1, -1, 0)]
WINDOW += [(0, 2), (0, 1), (0, -1)]
QUARTER = [6, -6, 2, -2]
HEADS = list(range(1, NH))
NEAR = [1, -1, 2, -2, 3, -3, 4, -4]
STAGES = 11


def kernel(
    hid_h, gain_h, wq_h, wk_h, wv_h, wo_h, down_h, up_h, choice_h, lengths_h, kc_h, vc_h,
    out,
    hid, gain, wq, wk, wv, wo, down, up, kc, vc, choice, lengths,
    t1a, t1b, flat, rsb_src, rsb, z2b, ups_src, ups, z2e, agq, rso_src, rso, z2o, ago, hbuf,
    load_sem, send_sem, recv_sem, vouch,
):
    seq = lax.axis_index("seq")
    head = lax.axis_index("head")
    y = lax.rem(seq, NY)
    z = lax.div(seq, NY)
    mine = y * 4 + lax.rem(z, 4)
    first = y * 4 + lax.rem(z + 2, 4)

    def at(dy, dz, dh):
        yy = lax.rem(y + (dy + NY) % NY, NY)
        zz = lax.rem(z + (dz + NZ) % NZ, NZ)
        return (zz * NY + yy, lax.rem(head + (dh + NH) % NH, NH))

    loads = [
        pltpu.make_async_copy(src, dst, load_sem.at[k])
        for k, (src, dst) in enumerate(
            [(hid_h, hid), (gain_h, gain), (down_h, down), (wq_h, wq), (wk_h, wk), (wv_h, wv),
             (up_h, up), (kc_h, kc), (vc_h, vc), (wo_h, wo), (choice_h, choice),
             (lengths_h, lengths)]
        )
    ]
    for k in (10, 0, 1, 2, 6, 3, 4, 5, 7, 8, 9, 11):
        loads[k].start()

    barrier = pltpu.get_barrier_semaphore()
    greeted = [(0, dz, 0) for dz in NEAR]
    greeted += [(-dy, -dz, 0) for dy, dz in WINDOW if dy and dz]
    greeted += [(dy, 0, dh) for dy, dh in PLANE]
    for dy, dz, dh in greeted:
        pl.semaphore_signal(barrier, inc=1, device_id=at(dy, dz, dh), device_id_type=MESH)

    def send(stage, src, dst, where):
        pltpu.make_async_remote_copy(
            src_ref=src, dst_ref=dst, send_sem=send_sem.at[stage], recv_sem=recv_sem.at[stage],
            device_id=at(*where), device_id_type=MESH,
        ).start()

    def bundle(stage, view):
        return pltpu.make_async_remote_copy(
            src_ref=view, dst_ref=view, send_sem=send_sem.at[stage], recv_sem=recv_sem.at[stage],
            device_id=at(0, 1, 0), device_id_type=MESH,
        )

    rows = lax.broadcasted_iota(jnp.int32, (16, 128), 0)
    lane = lax.broadcasted_iota(jnp.int32, (16, 128), 1)
    group = lane // 16
    rows8 = lax.rem(rows, 8)
    lane8 = lax.broadcasted_iota(jnp.int32, (8, 128), 1)
    loads[10].wait()
    chosen = jnp.zeros((16, 128), jnp.int32)
    for r in range(16):
        chosen = jnp.where(rows == r, choice[r], chosen)

    for c in loads[:3]:
        c.wait()
    values = hid[...].astype(F32)
    scaled = (values * gain[...].astype(F32)).astype(BF16)
    every = lax.dot_general(
        scaled, down[...], (((1,), (1,)), ((), ())), preferred_element_type=F32
    )
    fold = jnp.zeros((16, 128), F32)
    for j in range(8):
        fold += jnp.where(
            chosen == head * 64 + j * 8 + group, every[:, j * 128 : (j + 1) * 128], 0.0
        )
    for shift in (64, 32, 16):
        fold += pltpu.roll(fold, shift, 1)
    diagonal = jnp.where(group == rows8, fold, 0.0)
    square = jnp.sum(values * values, axis=1, keepdims=True)
    t1a[0, 0:1, :] = jnp.sum(diagonal[0:8], axis=0, keepdims=True)
    t1a[0, 1:2, :] = jnp.sum(diagonal[8:16], axis=0, keepdims=True)

    loads[6].wait()
    for r in range(16):
        local = choice[r] - seq * 8
        found = up[jnp.clip(local, 0, 7)]
        here = (chosen[r : r + 1] >= seq * 8) & (chosen[r : r + 1] < seq * 8 + 8)
        here = jnp.broadcast_to(jnp.where(here, 1.0, 0.0), (16, 128)).astype(BF16)
        for j in range(8):
            ups_src[r, :, j * 128 : (j + 1) * 128] = found[:, j * 128 : (j + 1) * 128] * here

    for c in loads[3:6]:
        c.wait()
    query_part = jnp.dot(scaled, wq[...], preferred_element_type=F32)
    key_part = jnp.dot(scaled, wk[...], preferred_element_type=F32)
    value_part = jnp.dot(scaled, wv[...], preferred_element_type=F32)
    for j in range(8):
        flat[pl.ds(j, 16, stride=16), :] = query_part[:, j * 128 : (j + 1) * 128]
    flat[pl.ds(8, 16, stride=16), :] = key_part
    flat[pl.ds(9, 16, stride=16), :] = value_part
    flat[pl.ds(10, 16, stride=16), :] = jnp.broadcast_to(square, (16, 128))
    for j in range(11, 16):
        flat[pl.ds(j, 16, stride=16), :] = jnp.zeros((16, 128), F32)
    rsb_src[...] = flat[...].reshape(16, 16, 128).astype(BF16)

    pl.semaphore_wait(barrier, len(greeted))
    for k, (dy, dh) in enumerate(PLANE):
        send(0, t1a.at[0], t1a.at[k + 1], (dy, 0, dh))
    for dz in (4, -4):
        pl.semaphore_signal(vouch, inc=1, device_id=at(0, dz, 0), device_id_type=MESH)

    def row_of(dy, dz):
        return lax.rem(y + dy, 4) * 4 + lax.rem(z + dz + 6, 4)

    for k, (dy, dz) in enumerate(WINDOW):
        send(2, rsb_src.at[row_of(dy, dz)], rsb.at[k], (dy, dz, 0))
    for k, (dy, dz) in enumerate(WINDOW):
        send(4, ups_src.at[row_of(dy, dz)], ups.at[k], (dy, dz, 0))

    bundle(0, t1a.at[1:32]).wait_recv()
    t1b[0] = jnp.sum(t1a[...], axis=0)
    pl.semaphore_wait(vouch, 2)
    for k, dz in enumerate(COLUMN):
        send(1, t1b.at[0], t1b.at[k + 1], (0, dz, 0))

    bundle(2, rsb).wait_recv()
    base = rsb_src[first].astype(F32)
    for k in range(15):
        base += rsb[k].astype(F32)
    z2b[0] = base.astype(BF16)
    for k, dz in enumerate(QUARTER):
        send(3, z2b.at[0], z2b.at[k + 1], (0, dz, 0))

    loads[11].wait()
    half = lax.rem(lane8, 64).astype(F32)
    frequency = jnp.exp(-half * (jnp.log(jnp.full((8, 128), rope_base, F32)) / 64.0))
    angle = lengths[mine].astype(F32) * frequency
    cosine = jnp.cos(angle)
    sine = jnp.sin(angle)
    sine = jnp.where(lane8 < 64, -sine, sine)

    bundle(4, ups).wait_recv()
    up_rows = ups_src[first]
    for k in range(15):
        up_rows += ups[k]
    bundle(1, t1b.at[1:16]).wait_recv()
    whole = jnp.sum(t1b[...], axis=0)
    ranks = jnp.where(first < 8, whole[0:1], whole[1:2])
    ranks = pltpu.roll(ranks, lax.rem(128 - 16 * lax.rem(first, 8), 128), 1)
    ranks = jnp.broadcast_to(ranks, (8, 128)).astype(BF16)
    expand = jnp.dot(ranks[:, 0:16], up_rows, preferred_element_type=F32)
    sub8 = lax.broadcasted_iota(jnp.int32, (8, 128), 0)
    grown = jnp.zeros((8, 128), F32)
    for j in range(8):
        grown += jnp.where(sub8 == j, expand[:, j * 128 : (j + 1) * 128], 0.0)
    z2e[0] = grown.astype(BF16)
    for k, dz in enumerate(QUARTER):
        send(5, z2e.at[0], z2e.at[k + 1], (0, dz, 0))

    bundle(3, z2b.at[1:5]).wait_recv()
    base = z2b[1].astype(F32)
    for k in range(2, 5):
        base += z2b[k].astype(F32)
    inverse = lax.rsqrt(base[10:11] * (1.0 / 8192.0) + norm_epsilon)

    def rotated(x):
        return (x * cosine + pltpu.roll(x, 64, 1) * sine).astype(BF16)

    key_rot = rotated(jnp.broadcast_to(base[8:9] * inverse, (8, 128))).astype(F32)
    value_own = jnp.broadcast_to(base[9:10] * inverse, (8, 128)).astype(BF16).astype(F32)
    bundle(5, z2e.at[1:5]).wait_recv()
    query = base[0:8]
    for k in range(1, 5):
        query += z2e[k].astype(F32)
    query_rot = rotated(query * inverse)
    agq[mine] = query_rot
    for dy, dz in WINDOW:
        send(6, agq.at[mine], agq.at[mine], (dy, dz, 0))
    scale = 128.0**-0.5
    own_score = jnp.sum(query_rot.astype(F32) * key_rot, axis=1, keepdims=True) * scale

    def packed(high, low, total, result):
        stat = jnp.where(lane8 < 32, high, jnp.where(lane8 < 64, low, total))
        return jnp.concatenate([result, stat], axis=0).astype(BF16)

    def merged(parts):
        parts = [part.astype(F32) for part in parts]
        stats = [part[8:16] for part in parts]
        tops = [
            jnp.broadcast_to(stat[:, 0:1] + stat[:, 32:33], (8, 128)) for stat in stats
        ]
        totals = [jnp.broadcast_to(stat[:, 64:65], (8, 128)) for stat in stats]
        top = tops[0]
        for t in tops[1:]:
            top = jnp.maximum(top, t)
        high = top.astype(BF16).astype(F32)
        low = (top - high).astype(BF16).astype(F32)
        total = jnp.zeros((8, 128), F32)
        result = jnp.zeros((8, 128), F32)
        for t, s, part in zip(tops, totals, parts):
            factor = jnp.exp(t - (high + low))
            total += s * factor
            result += part[0:8] * factor
        return high, low, total, result

    loads[7].wait()
    loads[8].wait()
    bundle(6, agq.at[0:15]).wait_recv()
    position = lax.broadcasted_iota(jnp.int32, (8, 256), 1) + seq * 256
    each = range(16)
    scores = [
        lax.dot_general(agq[r], kc[r], (((1,), (1,)), ((), ())), preferred_element_type=F32)
        * scale
        for r in each
    ]
    valid = [position < lengths[r] for r in each]
    scores = [jnp.where(valid[r], scores[r], masked_score) for r in each]
    tops = [jnp.max(scores[r], axis=1, keepdims=True) for r in each]
    highs = [top.astype(BF16).astype(F32) for top in tops]
    lows = [(top - high).astype(BF16).astype(F32) for top, high in zip(tops, highs)]
    weights = [
        jnp.where(valid[r], jnp.exp(scores[r] - (highs[r] + lows[r])), 0.0) for r in each
    ]
    totals = [jnp.sum(weights[r], axis=1, keepdims=True) for r in each]
    results = [
        jnp.dot(weights[r].astype(BF16), vc[r], preferred_element_type=F32) for r in each
    ]
    for r in each:
        rso_src[r] = packed(highs[r], lows[r], totals[r], results[r])
    for k, (dy, dz) in enumerate(WINDOW):
        send(7, rso_src.at[row_of(dy, dz)], rso.at[k], (dy, dz, 0))

    bundle(7, rso).wait_recv()
    z2o[0] = packed(*merged([rso_src[first]] + [rso[k] for k in range(15)]))
    for k, dz in enumerate(QUARTER):
        send(8, z2o.at[0], z2o.at[k + 1], (0, dz, 0))
    bundle(8, z2o.at[1:5]).wait_recv()
    high, low, total, result = merged([z2o[k] for k in range(1, 5)])
    top = high + low
    peak = jnp.maximum(top, own_score)
    factor = jnp.exp(top - peak)
    own_weight = jnp.exp(own_score - peak)
    attended = (result * factor + own_weight * value_own) / (total * factor + own_weight)
    ago[mine] = attended.astype(BF16)
    for dy, dz in WINDOW:
        send(9, ago.at[mine], ago.at[mine], (dy, dz, 0))

    loads[9].wait()
    bundle(9, ago.at[0:15]).wait_recv()
    flat[0:128, :] = ago[...].astype(F32).reshape(128, 128)
    projected = jnp.zeros((16, 128), F32)
    for j in range(8):
        projected += jnp.dot(
            flat[pl.ds(j, 16, stride=8), :].astype(BF16),
            wo[j * 128 : (j + 1) * 128, :],
            preferred_element_type=F32,
        )
    hbuf[0] = projected.astype(BF16)
    for k, dh in enumerate(HEADS):
        send(10, hbuf.at[0], hbuf.at[k + 1], (0, 0, dh))
    bundle(10, hbuf.at[1:8]).wait_recv()
    out[...] = jnp.sum(hbuf[...].astype(F32), axis=0).astype(BF16)

    for stage, view in enumerate(
        [t1a.at[1:32], t1b.at[1:16], rsb, z2b.at[1:5], ups, z2e.at[1:5], agq.at[0:15], rso,
         z2o.at[1:5], ago.at[0:15], hbuf.at[1:8]]
    ):
        bundle(stage, view).wait_send()


def body(hid, gain, wq, wk, wv, wo, down, up, choice, lengths, kc, vc):
    anywhere = pl.BlockSpec(memory_space=pl.ANY)
    return pl.pallas_call(
        kernel,
        out_shape=pltpu.VMEM((16, 128), BF16),
        in_specs=[anywhere] * 12,
        out_specs=pl.BlockSpec(memory_space=pltpu.VMEM),
        scratch_shapes=[
            pltpu.VMEM((16, 128), BF16),
            pltpu.VMEM((1, 128), BF16),
            pltpu.VMEM((128, 1024), BF16),
            pltpu.VMEM((128, 128), BF16),
            pltpu.VMEM((128, 128), BF16),
            pltpu.VMEM((1024, 128), BF16),
            pltpu.VMEM((1024, 128), BF16),
            pltpu.VMEM((8, 16, 1024), BF16),
            pltpu.VMEM((16, 256, 128), BF16),
            pltpu.VMEM((16, 256, 128), BF16),
            pltpu.SMEM((16,), jnp.int32),
            pltpu.SMEM((16,), jnp.int32),
            pltpu.VMEM((32, 2, 128), F32),
            pltpu.VMEM((16, 2, 128), F32),
            pltpu.VMEM((256, 128), F32),
            pltpu.VMEM((16, 16, 128), BF16),
            pltpu.VMEM((15, 16, 128), BF16),
            pltpu.VMEM((5, 16, 128), BF16),
            pltpu.VMEM((16, 16, 1024), BF16),
            pltpu.VMEM((15, 16, 1024), BF16),
            pltpu.VMEM((5, 8, 128), BF16),
            pltpu.VMEM((16, 8, 128), BF16),
            pltpu.VMEM((16, 16, 128), BF16),
            pltpu.VMEM((15, 16, 128), BF16),
            pltpu.VMEM((5, 16, 128), BF16),
            pltpu.VMEM((16, 8, 128), BF16),
            pltpu.VMEM((8, 16, 128), BF16),
            pltpu.SemaphoreType.DMA((12,)),
            pltpu.SemaphoreType.DMA((STAGES,)),
            pltpu.SemaphoreType.DMA((STAGES,)),
            pltpu.SemaphoreType.REGULAR,
        ],
        compiler_params=pltpu.CompilerParams(collective_id=0, has_side_effects=True),
    )(
        hid, gain.reshape(1, 128), wq, wk, wv, wo, down.reshape(1024, 128), up,
        choice, lengths, kc.reshape(16, 256, 128), vc.reshape(16, 256, 128),
    )


def solution(mesh):
    placed = (
        P(None, "seq"),
        P("seq"),
        P("seq", "head"),
        P("seq", "head"),
        P("seq", "head"),
        P("head", "seq"),
        P("head", None, "seq"),
        P("seq", None, "head"),
        P(),
        P(),
        P(None, "seq", "head", None),
        P(None, "seq", "head", None),
    )
    return jax.shard_map(
        body, mesh=mesh, in_specs=placed, out_specs=P(None, "seq"), check_vma=False
    )
```

```python
import jax
import jax.numpy as jnp
from jax import lax
from jax.experimental import pallas as pl
from jax.experimental.pallas import tpu as pltpu
from jax.sharding import PartitionSpec as P

MESH = pl.DeviceIdType.MESH
F32 = jnp.float32
BF16 = jnp.bfloat16

norm_epsilon = 1e-05
rope_base = 500000.0
masked_score = -1e30

NY, NZ, NH = 4, 16, 8
PLANE = [(dy, dh) for dy in range(NY) for dh in range(NH) if (dy, dh) != (0, 0)]
COLUMN = list(range(1, NZ))
WINDOW = [(2, 1), (2, -1), (-1, 2), (-1, -2), (2, 0), (1, 1), (1, -1), (-1, 1), (-1, -1)]
WINDOW += [(0, 2), (0, -2), (1, 0), (-1, 0), (0, 1), (0, -1)]
QUARTER = [(-1, 6), (1, -6), (1, 2), (-1, -2)]
HEADS = list(range(1, NH))
NEAR = [1, -1, 2, -2, 3, -3, 4, -4]
STAGES = 11


def kernel(
    hid_h, gain_h, wq_h, wk_h, wv_h, wo_h, down_h, up_h, choice_h, lengths_h, kc_h, vc_h,
    out,
    hid, gain, wq, wk, wv, wo, down, up, kc, vc, choice, lengths,
    t1a, t1b, flat, rsb_src, rsb, z2b, ups_src, ups, z2e, agq, rso_src, rso, z2o, ago, hbuf,
    load_sem, send_sem, recv_sem, vouch,
):
    seq = lax.axis_index("seq")
    head = lax.axis_index("head")
    y = lax.rem(seq, NY)
    z = lax.div(seq, NY)

    def owned(dy, dz):
        zz = lax.rem(z + dz + NZ, NZ)
        return lax.rem(y + dy + NY + 2 * lax.div(zz, 4), 4) * 4 + lax.rem(zz, 4)

    mine = owned(0, 0)
    first = owned(1, 2)

    def at(dy, dz, dh):
        yy = lax.rem(y + (dy + NY) % NY, NY)
        zz = lax.rem(z + (dz + NZ) % NZ, NZ)
        return (zz * NY + yy, lax.rem(head + (dh + NH) % NH, NH))

    loads = [
        pltpu.make_async_copy(src, dst, load_sem.at[k])
        for k, (src, dst) in enumerate(
            [(hid_h, hid), (gain_h, gain), (down_h, down), (wq_h, wq), (wk_h, wk), (wv_h, wv),
             (up_h, up), (kc_h, kc), (vc_h, vc), (wo_h, wo), (choice_h, choice),
             (lengths_h, lengths)]
        )
    ]
    for k in (10, 0, 1, 2, 6, 3, 4, 5, 7, 8, 9, 11):
        loads[k].start()

    barrier = pltpu.get_barrier_semaphore()
    greeted = [(0, dz, 0) for dz in NEAR]
    greeted += [(-dy, -dz, 0) for dy, dz in WINDOW if dy and dz]
    greeted += [(-1, 2, 0), (-1, -2, 0)]
    greeted += [(dy, 0, dh) for dy, dh in PLANE]
    for dy, dz, dh in greeted:
        pl.semaphore_signal(barrier, inc=1, device_id=at(dy, dz, dh), device_id_type=MESH)

    def send(stage, src, dst, where):
        pltpu.make_async_remote_copy(
            src_ref=src, dst_ref=dst, send_sem=send_sem.at[stage], recv_sem=recv_sem.at[stage],
            device_id=at(*where), device_id_type=MESH,
        ).start()

    def bundle(stage, view):
        return pltpu.make_async_remote_copy(
            src_ref=view, dst_ref=view, send_sem=send_sem.at[stage], recv_sem=recv_sem.at[stage],
            device_id=at(0, 1, 0), device_id_type=MESH,
        )

    rows = lax.broadcasted_iota(jnp.int32, (16, 128), 0)
    lane = lax.broadcasted_iota(jnp.int32, (16, 128), 1)
    group = lane // 16
    rows8 = lax.rem(rows, 8)
    lane8 = lax.broadcasted_iota(jnp.int32, (8, 128), 1)
    loads[10].wait()
    chosen = jnp.zeros((16, 128), jnp.int32)
    for r in range(16):
        chosen = jnp.where(rows == r, choice[r], chosen)

    for c in loads[:3]:
        c.wait()
    values = hid[...].astype(F32)
    scaled = (values * gain[...].astype(F32)).astype(BF16)
    every = lax.dot_general(
        scaled, down[...], (((1,), (1,)), ((), ())), preferred_element_type=F32
    )
    fold = jnp.zeros((16, 128), F32)
    for j in range(8):
        fold += jnp.where(
            chosen == head * 64 + j * 8 + group, every[:, j * 128 : (j + 1) * 128], 0.0
        )
    for shift in (64, 32, 16):
        fold += pltpu.roll(fold, shift, 1)
    diagonal = jnp.where(group == rows8, fold, 0.0)
    square = jnp.sum(values * values, axis=1, keepdims=True)
    t1a[0, 0:1, :] = jnp.sum(diagonal[0:8], axis=0, keepdims=True)
    t1a[0, 1:2, :] = jnp.sum(diagonal[8:16], axis=0, keepdims=True)

    loads[6].wait()
    for r in range(16):
        local = choice[r] - seq * 8
        found = up[jnp.clip(local, 0, 7)]
        here = (chosen[r : r + 1] >= seq * 8) & (chosen[r : r + 1] < seq * 8 + 8)
        here = jnp.broadcast_to(jnp.where(here, 1.0, 0.0), (16, 128)).astype(BF16)
        for j in range(8):
            ups_src[r, :, j * 128 : (j + 1) * 128] = found[:, j * 128 : (j + 1) * 128] * here

    for c in loads[3:6]:
        c.wait()
    query_part = jnp.dot(scaled, wq[...], preferred_element_type=F32)
    key_part = jnp.dot(scaled, wk[...], preferred_element_type=F32)
    value_part = jnp.dot(scaled, wv[...], preferred_element_type=F32)
    for j in range(8):
        flat[pl.ds(j, 16, stride=16), :] = query_part[:, j * 128 : (j + 1) * 128]
    flat[pl.ds(8, 16, stride=16), :] = key_part
    flat[pl.ds(9, 16, stride=16), :] = value_part
    flat[pl.ds(10, 16, stride=16), :] = jnp.broadcast_to(square, (16, 128))
    for j in range(11, 16):
        flat[pl.ds(j, 16, stride=16), :] = jnp.zeros((16, 128), F32)
    rsb_src[...] = flat[...].reshape(16, 16, 128).astype(BF16)

    pl.semaphore_wait(barrier, len(greeted))
    for k, (dy, dh) in enumerate(PLANE):
        send(0, t1a.at[0], t1a.at[k + 1], (dy, 0, dh))
    for dz in (4, -4):
        pl.semaphore_signal(vouch, inc=1, device_id=at(0, dz, 0), device_id_type=MESH)

    def row_of(dy, dz):
        return owned(dy + 1, dz + 2)

    for k, (dy, dz) in enumerate(WINDOW):
        send(2, rsb_src.at[row_of(dy, dz)], rsb.at[k], (dy, dz, 0))
    for k, (dy, dz) in enumerate(WINDOW):
        send(4, ups_src.at[row_of(dy, dz)], ups.at[k], (dy, dz, 0))

    bundle(0, t1a.at[1:32]).wait_recv()
    t1b[0] = jnp.sum(t1a[...], axis=0)
    pl.semaphore_wait(vouch, 2)
    for k, dz in enumerate(COLUMN):
        send(1, t1b.at[0], t1b.at[k + 1], (0, dz, 0))

    bundle(2, rsb).wait_recv()
    base = rsb_src[first].astype(F32)
    for k in range(15):
        base += rsb[k].astype(F32)
    z2b[0] = base.astype(BF16)
    for k, (dy, dz) in enumerate(QUARTER):
        send(3, z2b.at[0], z2b.at[k + 1], (dy, dz, 0))

    loads[11].wait()
    half = lax.rem(lane8, 64).astype(F32)
    frequency = jnp.exp(-half * (jnp.log(jnp.full((8, 128), rope_base, F32)) / 64.0))
    angle = lengths[mine].astype(F32) * frequency
    cosine = jnp.cos(angle)
    sine = jnp.sin(angle)
    sine = jnp.where(lane8 < 64, -sine, sine)

    bundle(4, ups).wait_recv()
    up_rows = ups_src[first]
    for k in range(15):
        up_rows += ups[k]
    bundle(1, t1b.at[1:16]).wait_recv()
    whole = jnp.sum(t1b[...], axis=0)
    ranks = jnp.where(first < 8, whole[0:1], whole[1:2])
    ranks = pltpu.roll(ranks, lax.rem(128 - 16 * lax.rem(first, 8), 128), 1)
    ranks = jnp.broadcast_to(ranks, (8, 128)).astype(BF16)
    expand = jnp.dot(ranks[:, 0:16], up_rows, preferred_element_type=F32)
    sub8 = lax.broadcasted_iota(jnp.int32, (8, 128), 0)
    grown = jnp.zeros((8, 128), F32)
    for j in range(8):
        grown += jnp.where(sub8 == j, expand[:, j * 128 : (j + 1) * 128], 0.0)
    z2e[0] = grown.astype(BF16)
    for k, (dy, dz) in enumerate(QUARTER):
        send(5, z2e.at[0], z2e.at[k + 1], (dy, dz, 0))

    bundle(3, z2b.at[1:5]).wait_recv()
    base = z2b[1].astype(F32)
    for k in range(2, 5):
        base += z2b[k].astype(F32)
    inverse = lax.rsqrt(base[10:11] * (1.0 / 8192.0) + norm_epsilon)

    def rotated(x):
        return (x * cosine + pltpu.roll(x, 64, 1) * sine).astype(BF16)

    key_rot = rotated(jnp.broadcast_to(base[8:9] * inverse, (8, 128))).astype(F32)
    value_own = jnp.broadcast_to(base[9:10] * inverse, (8, 128)).astype(BF16).astype(F32)
    bundle(5, z2e.at[1:5]).wait_recv()
    query = base[0:8]
    for k in range(1, 5):
        query += z2e[k].astype(F32)
    query_rot = rotated(query * inverse)
    agq[mine] = query_rot
    for dy, dz in WINDOW:
        send(6, agq.at[mine], agq.at[mine], (dy, dz, 0))
    scale = 128.0**-0.5
    own_score = jnp.sum(query_rot.astype(F32) * key_rot, axis=1, keepdims=True) * scale

    def packed(high, low, total, result):
        stat = jnp.where(lane8 < 32, high, jnp.where(lane8 < 64, low, total))
        return jnp.concatenate([result, stat], axis=0).astype(BF16)

    def merged(parts):
        parts = [part.astype(F32) for part in parts]
        stats = [part[8:16] for part in parts]
        tops = [
            jnp.broadcast_to(stat[:, 0:1] + stat[:, 32:33], (8, 128)) for stat in stats
        ]
        totals = [jnp.broadcast_to(stat[:, 64:65], (8, 128)) for stat in stats]
        top = tops[0]
        for t in tops[1:]:
            top = jnp.maximum(top, t)
        high = top.astype(BF16).astype(F32)
        low = (top - high).astype(BF16).astype(F32)
        total = jnp.zeros((8, 128), F32)
        result = jnp.zeros((8, 128), F32)
        for t, s, part in zip(tops, totals, parts):
            factor = jnp.exp(t - (high + low))
            total += s * factor
            result += part[0:8] * factor
        return high, low, total, result

    loads[7].wait()
    loads[8].wait()
    bundle(6, agq.at[0:15]).wait_recv()
    position = lax.broadcasted_iota(jnp.int32, (8, 256), 1) + seq * 256
    each = range(16)
    scores = [
        lax.dot_general(agq[r], kc[r], (((1,), (1,)), ((), ())), preferred_element_type=F32)
        * scale
        for r in each
    ]
    valid = [position < lengths[r] for r in each]
    scores = [jnp.where(valid[r], scores[r], masked_score) for r in each]
    tops = [jnp.max(scores[r], axis=1, keepdims=True) for r in each]
    highs = [top.astype(BF16).astype(F32) for top in tops]
    lows = [(top - high).astype(BF16).astype(F32) for top, high in zip(tops, highs)]
    weights = [
        jnp.where(valid[r], jnp.exp(scores[r] - (highs[r] + lows[r])), 0.0) for r in each
    ]
    totals = [jnp.sum(weights[r], axis=1, keepdims=True) for r in each]
    results = [
        jnp.dot(weights[r].astype(BF16), vc[r], preferred_element_type=F32) for r in each
    ]
    for r in each:
        rso_src[r] = packed(highs[r], lows[r], totals[r], results[r])
    for k, (dy, dz) in enumerate(WINDOW):
        send(7, rso_src.at[row_of(dy, dz)], rso.at[k], (dy, dz, 0))

    bundle(7, rso).wait_recv()
    z2o[0] = packed(*merged([rso_src[first]] + [rso[k] for k in range(15)]))
    for k, (dy, dz) in enumerate(QUARTER):
        send(8, z2o.at[0], z2o.at[k + 1], (dy, dz, 0))
    bundle(8, z2o.at[1:5]).wait_recv()
    high, low, total, result = merged([z2o[k] for k in range(1, 5)])
    top = high + low
    peak = jnp.maximum(top, own_score)
    factor = jnp.exp(top - peak)
    own_weight = jnp.exp(own_score - peak)
    attended = (result * factor + own_weight * value_own) / (total * factor + own_weight)
    ago[mine] = attended.astype(BF16)
    for dy, dz in WINDOW:
        send(9, ago.at[mine], ago.at[mine], (dy, dz, 0))

    loads[9].wait()
    bundle(9, ago.at[0:15]).wait_recv()
    flat[0:128, :] = ago[...].astype(F32).reshape(128, 128)
    projected = jnp.zeros((16, 128), F32)
    for j in range(8):
        projected += jnp.dot(
            flat[pl.ds(j, 16, stride=8), :].astype(BF16),
            wo[j * 128 : (j + 1) * 128, :],
            preferred_element_type=F32,
        )
    hbuf[0] = projected.astype(BF16)
    for k, dh in enumerate(HEADS):
        send(10, hbuf.at[0], hbuf.at[k + 1], (0, 0, dh))
    bundle(10, hbuf.at[1:8]).wait_recv()
    out[...] = jnp.sum(hbuf[...].astype(F32), axis=0).astype(BF16)

    for stage, view in enumerate(
        [t1a.at[1:32], t1b.at[1:16], rsb, z2b.at[1:5], ups, z2e.at[1:5], agq.at[0:15], rso,
         z2o.at[1:5], ago.at[0:15], hbuf.at[1:8]]
    ):
        bundle(stage, view).wait_send()


def body(hid, gain, wq, wk, wv, wo, down, up, choice, lengths, kc, vc):
    anywhere = pl.BlockSpec(memory_space=pl.ANY)
    return pl.pallas_call(
        kernel,
        out_shape=pltpu.VMEM((16, 128), BF16),
        in_specs=[anywhere] * 12,
        out_specs=pl.BlockSpec(memory_space=pltpu.VMEM),
        scratch_shapes=[
            pltpu.VMEM((16, 128), BF16),
            pltpu.VMEM((1, 128), BF16),
            pltpu.VMEM((128, 1024), BF16),
            pltpu.VMEM((128, 128), BF16),
            pltpu.VMEM((128, 128), BF16),
            pltpu.VMEM((1024, 128), BF16),
            pltpu.VMEM((1024, 128), BF16),
            pltpu.VMEM((8, 16, 1024), BF16),
            pltpu.VMEM((16, 256, 128), BF16),
            pltpu.VMEM((16, 256, 128), BF16),
            pltpu.SMEM((16,), jnp.int32),
            pltpu.SMEM((16,), jnp.int32),
            pltpu.VMEM((32, 2, 128), F32),
            pltpu.VMEM((16, 2, 128), F32),
            pltpu.VMEM((256, 128), F32),
            pltpu.VMEM((16, 16, 128), BF16),
            pltpu.VMEM((15, 16, 128), BF16),
            pltpu.VMEM((5, 16, 128), BF16),
            pltpu.VMEM((16, 16, 1024), BF16),
            pltpu.VMEM((15, 16, 1024), BF16),
            pltpu.VMEM((5, 8, 128), BF16),
            pltpu.VMEM((16, 8, 128), BF16),
            pltpu.VMEM((16, 16, 128), BF16),
            pltpu.VMEM((15, 16, 128), BF16),
            pltpu.VMEM((5, 16, 128), BF16),
            pltpu.VMEM((16, 8, 128), BF16),
            pltpu.VMEM((8, 16, 128), BF16),
            pltpu.SemaphoreType.DMA((12,)),
            pltpu.SemaphoreType.DMA((STAGES,)),
            pltpu.SemaphoreType.DMA((STAGES,)),
            pltpu.SemaphoreType.REGULAR,
        ],
        compiler_params=pltpu.CompilerParams(collective_id=0, has_side_effects=True),
    )(
        hid, gain.reshape(1, 128), wq, wk, wv, wo, down.reshape(1024, 128), up,
        choice, lengths, kc.reshape(16, 256, 128), vc.reshape(16, 256, 128),
    )


def solution(mesh):
    placed = (
        P(None, "seq"),
        P("seq"),
        P("seq", "head"),
        P("seq", "head"),
        P("seq", "head"),
        P("head", "seq"),
        P("head", None, "seq"),
        P("seq", None, "head"),
        P(),
        P(),
        P(None, "seq", "head", None),
        P(None, "seq", "head", None),
    )
    return jax.shard_map(
        body, mesh=mesh, in_specs=placed, out_specs=P(None, "seq"), check_vma=False
    )
```

```python
import jax
import jax.numpy as jnp
from jax import lax
from jax.experimental import pallas as pl
from jax.experimental.pallas import tpu as pltpu
from jax.sharding import PartitionSpec as P

MESH = pl.DeviceIdType.MESH
F32 = jnp.float32
BF16 = jnp.bfloat16

norm_epsilon = 1e-05
rope_base = 500000.0
masked_score = -1e30

NY, NZ, NH = 4, 16, 8
PLANE = [(dy, dh) for dy in range(NY) for dh in range(NH) if (dy, dh) != (0, 0)]
COLUMN = list(range(1, NZ))
WINDOW = [(dy, dz) for dy in (2, 1, 3) for dz in (2 if dy == 2 else -2, 1, -1, 0)]
WINDOW += [(0, 2), (0, 1), (0, -1)]
QUARTER = [6, -6, 2, -2]
HEADS = list(range(1, NH))
NEAR = [1, -1, 2, -2, 3, -3, 4, -4]
STAGES = 12


def kernel(
    hid_h, gain_h, wq_h, wk_h, wv_h, wo_h, down_h, up_h, choice_h, lengths_h, kc_h, vc_h,
    out,
    hid, gain, wq, wk, wv, wo, down, up, kc, vc, choice, lengths,
    t1a, t1b, flat, rsb_src, rsb, z2b, ups_src, ups, ups_y, z2e, agq, rso_src, rso, z2o, ago, hbuf,
    load_sem, send_sem, recv_sem, vouch,
):
    seq = lax.axis_index("seq")
    head = lax.axis_index("head")
    y = lax.rem(seq, NY)
    z = lax.div(seq, NY)
    mine = y * 4 + lax.rem(z, 4)
    first = y * 4 + lax.rem(z + 2, 4)

    def at(dy, dz, dh):
        yy = lax.rem(y + (dy + NY) % NY, NY)
        zz = lax.rem(z + (dz + NZ) % NZ, NZ)
        return (zz * NY + yy, lax.rem(head + (dh + NH) % NH, NH))

    loads = [
        pltpu.make_async_copy(src, dst, load_sem.at[k])
        for k, (src, dst) in enumerate(
            [(hid_h, hid), (gain_h, gain), (down_h, down), (wq_h, wq), (wk_h, wk), (wv_h, wv),
             (up_h, up), (kc_h, kc), (vc_h, vc), (wo_h, wo), (choice_h, choice),
             (lengths_h, lengths)]
        )
    ]
    for k in (10, 0, 1, 2, 6, 3, 4, 5, 7, 8, 9, 11):
        loads[k].start()

    barrier = pltpu.get_barrier_semaphore()
    greeted = [(0, dz, 0) for dz in NEAR]
    greeted += [(-dy, -dz, 0) for dy, dz in WINDOW if dy and dz]
    greeted += [(dy, 0, dh) for dy, dh in PLANE]
    for dy, dz, dh in greeted:
        pl.semaphore_signal(barrier, inc=1, device_id=at(dy, dz, dh), device_id_type=MESH)

    def send(stage, src, dst, where):
        pltpu.make_async_remote_copy(
            src_ref=src, dst_ref=dst, send_sem=send_sem.at[stage], recv_sem=recv_sem.at[stage],
            device_id=at(*where), device_id_type=MESH,
        ).start()

    def bundle(stage, view):
        return pltpu.make_async_remote_copy(
            src_ref=view, dst_ref=view, send_sem=send_sem.at[stage], recv_sem=recv_sem.at[stage],
            device_id=at(0, 1, 0), device_id_type=MESH,
        )

    rows = lax.broadcasted_iota(jnp.int32, (16, 128), 0)
    lane = lax.broadcasted_iota(jnp.int32, (16, 128), 1)
    group = lane // 16
    rows8 = lax.rem(rows, 8)
    lane8 = lax.broadcasted_iota(jnp.int32, (8, 128), 1)
    loads[10].wait()
    chosen = jnp.zeros((16, 128), jnp.int32)
    for r in range(16):
        chosen = jnp.where(rows == r, choice[r], chosen)

    for c in loads[:3]:
        c.wait()
    values = hid[...].astype(F32)
    scaled = (values * gain[...].astype(F32)).astype(BF16)
    every = lax.dot_general(
        scaled, down[...], (((1,), (1,)), ((), ())), preferred_element_type=F32
    )
    fold = jnp.zeros((16, 128), F32)
    for j in range(8):
        fold += jnp.where(
            chosen == head * 64 + j * 8 + group, every[:, j * 128 : (j + 1) * 128], 0.0
        )
    for shift in (64, 32, 16):
        fold += pltpu.roll(fold, shift, 1)
    diagonal = jnp.where(group == rows8, fold, 0.0)
    square = jnp.sum(values * values, axis=1, keepdims=True)
    t1a[0, 0:1, :] = jnp.sum(diagonal[0:8], axis=0, keepdims=True)
    t1a[0, 1:2, :] = jnp.sum(diagonal[8:16], axis=0, keepdims=True)

    loads[6].wait()
    for r in range(16):
        local = choice[r] - seq * 8
        found = up[jnp.clip(local, 0, 7)]
        here = (chosen[r : r + 1] >= seq * 8) & (chosen[r : r + 1] < seq * 8 + 8)
        here = jnp.broadcast_to(jnp.where(here, 1.0, 0.0), (16, 128)).astype(BF16)
        for j in range(8):
            ups_src[r % 4, r // 4, :, j * 128 : (j + 1) * 128] = found[:, j * 128 : (j + 1) * 128] * here

    for c in loads[3:6]:
        c.wait()
    query_part = jnp.dot(scaled, wq[...], preferred_element_type=F32)
    key_part = jnp.dot(scaled, wk[...], preferred_element_type=F32)
    value_part = jnp.dot(scaled, wv[...], preferred_element_type=F32)
    for j in range(8):
        flat[pl.ds(j, 16, stride=16), :] = query_part[:, j * 128 : (j + 1) * 128]
    flat[pl.ds(8, 16, stride=16), :] = key_part
    flat[pl.ds(9, 16, stride=16), :] = value_part
    flat[pl.ds(10, 16, stride=16), :] = jnp.broadcast_to(square, (16, 128))
    for j in range(11, 16):
        flat[pl.ds(j, 16, stride=16), :] = jnp.zeros((16, 128), F32)
    rsb_src[...] = flat[...].reshape(16, 16, 128).astype(BF16)

    pl.semaphore_wait(barrier, len(greeted))
    for k, (dy, dh) in enumerate(PLANE):
        send(0, t1a.at[0], t1a.at[k + 1], (dy, 0, dh))
    for dz in (4, -4):
        pl.semaphore_signal(vouch, inc=1, device_id=at(0, dz, 0), device_id_type=MESH)

    def row_of(dy, dz):
        return lax.rem(y + dy, 4) * 4 + lax.rem(z + dz + 6, 4)

    for k, (dy, dz) in enumerate(WINDOW):
        send(2, rsb_src.at[row_of(dy, dz)], rsb.at[k], (dy, dz, 0))
    for dz, k, low, high in ((2, 2, 0, 2), (-2, 2, 2, 4), (1, 0, 0, 4), (-1, 1, 0, 4)):
        part = ups_src.at[lax.rem(z + dz + 2, 4), low:high]
        send(4, part, ups.at[k, low:high], (0, dz, 0))

    bundle(0, t1a.at[1:32]).wait_recv()
    t1b[0] = jnp.sum(t1a[...], axis=0)
    pl.semaphore_wait(vouch, 2)
    for k, dz in enumerate(COLUMN):
        send(1, t1b.at[0], t1b.at[k + 1], (0, dz, 0))

    bundle(2, rsb).wait_recv()
    base = rsb_src[first].astype(F32)
    for k in range(15):
        base += rsb[k].astype(F32)
    z2b[0] = base.astype(BF16)
    for k, dz in enumerate(QUARTER):
        send(3, z2b.at[0], z2b.at[k + 1], (0, dz, 0))

    bundle(4, ups).wait_recv()
    ups_y[0] = (ups_src[lax.rem(z + 2, 4)] + ups[0]) + (ups[1] + ups[2])
    for dy in (2, 1, 3):
        send(11, ups_y.at[0, lax.rem(y + dy, 4)], ups_y.at[1, dy], (dy, 0, 0))

    loads[11].wait()
    half = lax.rem(lane8, 64).astype(F32)
    frequency = jnp.exp(-half * (jnp.log(jnp.full((8, 128), rope_base, F32)) / 64.0))
    angle = lengths[mine].astype(F32) * frequency
    cosine = jnp.cos(angle)
    sine = jnp.sin(angle)
    sine = jnp.where(lane8 < 64, -sine, sine)

    bundle(11, ups_y.at[1, 1:4]).wait_recv()
    up_rows = (ups_y[0, y] + ups_y[1, 1]) + (ups_y[1, 2] + ups_y[1, 3])
    bundle(1, t1b.at[1:16]).wait_recv()
    whole = jnp.sum(t1b[...], axis=0)
    ranks = jnp.where(first < 8, whole[0:1], whole[1:2])
    ranks = pltpu.roll(ranks, lax.rem(128 - 16 * lax.rem(first, 8), 128), 1)
    ranks = jnp.broadcast_to(ranks, (8, 128)).astype(BF16)
    expand = jnp.dot(ranks[:, 0:16], up_rows, preferred_element_type=F32)
    sub8 = lax.broadcasted_iota(jnp.int32, (8, 128), 0)
    grown = jnp.zeros((8, 128), F32)
    for j in range(8):
        grown += jnp.where(sub8 == j, expand[:, j * 128 : (j + 1) * 128], 0.0)
    z2e[0] = grown.astype(BF16)
    for k, dz in enumerate(QUARTER):
        send(5, z2e.at[0], z2e.at[k + 1], (0, dz, 0))

    bundle(3, z2b.at[1:5]).wait_recv()
    base = z2b[1].astype(F32)
    for k in range(2, 5):
        base += z2b[k].astype(F32)
    inverse = lax.rsqrt(base[10:11] * (1.0 / 8192.0) + norm_epsilon)

    def rotated(x):
        return (x * cosine + pltpu.roll(x, 64, 1) * sine).astype(BF16)

    key_rot = rotated(jnp.broadcast_to(base[8:9] * inverse, (8, 128))).astype(F32)
    value_own = jnp.broadcast_to(base[9:10] * inverse, (8, 128)).astype(BF16).astype(F32)
    bundle(5, z2e.at[1:5]).wait_recv()
    query = base[0:8]
    for k in range(1, 5):
        query += z2e[k].astype(F32)
    query_rot = rotated(query * inverse)
    agq[mine] = query_rot
    for dy, dz in WINDOW:
        send(6, agq.at[mine], agq.at[mine], (dy, dz, 0))
    scale = 128.0**-0.5
    own_score = jnp.sum(query_rot.astype(F32) * key_rot, axis=1, keepdims=True) * scale

    def packed(high, low, total, result):
        stat = jnp.where(lane8 < 32, high, jnp.where(lane8 < 64, low, total))
        return jnp.concatenate([result, stat], axis=0).astype(BF16)

    def merged(parts):
        parts = [part.astype(F32) for part in parts]
        stats = [part[8:16] for part in parts]
        tops = [
            jnp.broadcast_to(stat[:, 0:1] + stat[:, 32:33], (8, 128)) for stat in stats
        ]
        totals = [jnp.broadcast_to(stat[:, 64:65], (8, 128)) for stat in stats]
        top = tops[0]
        for t in tops[1:]:
            top = jnp.maximum(top, t)
        high = top.astype(BF16).astype(F32)
        low = (top - high).astype(BF16).astype(F32)
        total = jnp.zeros((8, 128), F32)
        result = jnp.zeros((8, 128), F32)
        for t, s, part in zip(tops, totals, parts):
            factor = jnp.exp(t - (high + low))
            total += s * factor
            result += part[0:8] * factor
        return high, low, total, result

    loads[7].wait()
    loads[8].wait()
    bundle(6, agq.at[0:15]).wait_recv()
    position = lax.broadcasted_iota(jnp.int32, (8, 256), 1) + seq * 256
    each = range(16)
    scores = [
        lax.dot_general(agq[r], kc[r], (((1,), (1,)), ((), ())), preferred_element_type=F32)
        * scale
        for r in each
    ]
    valid = [position < lengths[r] for r in each]
    scores = [jnp.where(valid[r], scores[r], masked_score) for r in each]
    tops = [jnp.max(scores[r], axis=1, keepdims=True) for r in each]
    highs = [top.astype(BF16).astype(F32) for top in tops]
    lows = [(top - high).astype(BF16).astype(F32) for top, high in zip(tops, highs)]
    weights = [
        jnp.where(valid[r], jnp.exp(scores[r] - (highs[r] + lows[r])), 0.0) for r in each
    ]
    totals = [jnp.sum(weights[r], axis=1, keepdims=True) for r in each]
    results = [
        jnp.dot(weights[r].astype(BF16), vc[r], preferred_element_type=F32) for r in each
    ]
    for r in each:
        rso_src[r] = packed(highs[r], lows[r], totals[r], results[r])
    for k, (dy, dz) in enumerate(WINDOW):
        send(7, rso_src.at[row_of(dy, dz)], rso.at[k], (dy, dz, 0))

    bundle(7, rso).wait_recv()
    z2o[0] = packed(*merged([rso_src[first]] + [rso[k] for k in range(15)]))
    for k, dz in enumerate(QUARTER):
        send(8, z2o.at[0], z2o.at[k + 1], (0, dz, 0))
    bundle(8, z2o.at[1:5]).wait_recv()
    high, low, total, result = merged([z2o[k] for k in range(1, 5)])
    top = high + low
    peak = jnp.maximum(top, own_score)
    factor = jnp.exp(top - peak)
    own_weight = jnp.exp(own_score - peak)
    attended = (result * factor + own_weight * value_own) / (total * factor + own_weight)
    ago[mine] = attended.astype(BF16)
    for dy, dz in WINDOW:
        send(9, ago.at[mine], ago.at[mine], (dy, dz, 0))

    loads[9].wait()
    bundle(9, ago.at[0:15]).wait_recv()
    flat[0:128, :] = ago[...].astype(F32).reshape(128, 128)
    projected = jnp.zeros((16, 128), F32)
    for j in range(8):
        projected += jnp.dot(
            flat[pl.ds(j, 16, stride=8), :].astype(BF16),
            wo[j * 128 : (j + 1) * 128, :],
            preferred_element_type=F32,
        )
    hbuf[0] = projected.astype(BF16)
    for k, dh in enumerate(HEADS):
        send(10, hbuf.at[0], hbuf.at[k + 1], (0, 0, dh))
    bundle(10, hbuf.at[1:8]).wait_recv()
    out[...] = jnp.sum(hbuf[...].astype(F32), axis=0).astype(BF16)

    for stage, view in enumerate(
        [t1a.at[1:32], t1b.at[1:16], rsb, z2b.at[1:5], ups, z2e.at[1:5], agq.at[0:15], rso,
         z2o.at[1:5], ago.at[0:15], hbuf.at[1:8],
         ups_y.at[1, 1:4]]
    ):
        bundle(stage, view).wait_send()


def body(hid, gain, wq, wk, wv, wo, down, up, choice, lengths, kc, vc):
    anywhere = pl.BlockSpec(memory_space=pl.ANY)
    return pl.pallas_call(
        kernel,
        out_shape=pltpu.VMEM((16, 128), BF16),
        in_specs=[anywhere] * 12,
        out_specs=pl.BlockSpec(memory_space=pltpu.VMEM),
        scratch_shapes=[
            pltpu.VMEM((16, 128), BF16),
            pltpu.VMEM((1, 128), BF16),
            pltpu.VMEM((128, 1024), BF16),
            pltpu.VMEM((128, 128), BF16),
            pltpu.VMEM((128, 128), BF16),
            pltpu.VMEM((1024, 128), BF16),
            pltpu.VMEM((1024, 128), BF16),
            pltpu.VMEM((8, 16, 1024), BF16),
            pltpu.VMEM((16, 256, 128), BF16),
            pltpu.VMEM((16, 256, 128), BF16),
            pltpu.SMEM((16,), jnp.int32),
            pltpu.SMEM((16,), jnp.int32),
            pltpu.VMEM((32, 2, 128), F32),
            pltpu.VMEM((16, 2, 128), F32),
            pltpu.VMEM((256, 128), F32),
            pltpu.VMEM((16, 16, 128), BF16),
            pltpu.VMEM((15, 16, 128), BF16),
            pltpu.VMEM((5, 16, 128), BF16),
            pltpu.VMEM((4, 4, 16, 1024), BF16),
            pltpu.VMEM((3, 4, 16, 1024), BF16),
            pltpu.VMEM((2, 4, 16, 1024), BF16),
            pltpu.VMEM((5, 8, 128), BF16),
            pltpu.VMEM((16, 8, 128), BF16),
            pltpu.VMEM((16, 16, 128), BF16),
            pltpu.VMEM((15, 16, 128), BF16),
            pltpu.VMEM((5, 16, 128), BF16),
            pltpu.VMEM((16, 8, 128), BF16),
            pltpu.VMEM((8, 16, 128), BF16),
            pltpu.SemaphoreType.DMA((12,)),
            pltpu.SemaphoreType.DMA((STAGES,)),
            pltpu.SemaphoreType.DMA((STAGES,)),
            pltpu.SemaphoreType.REGULAR,
        ],
        compiler_params=pltpu.CompilerParams(collective_id=0, has_side_effects=True),
    )(
        hid, gain.reshape(1, 128), wq, wk, wv, wo, down.reshape(1024, 128), up,
        choice, lengths, kc.reshape(16, 256, 128), vc.reshape(16, 256, 128),
    )


def solution(mesh):
    placed = (
        P(None, "seq"),
        P("seq"),
        P("seq", "head"),
        P("seq", "head"),
        P("seq", "head"),
        P("head", "seq"),
        P("head", None, "seq"),
        P("seq", None, "head"),
        P(),
        P(),
        P(None, "seq", "head", None),
        P(None, "seq", "head", None),
    )
    return jax.shard_map(
        body, mesh=mesh, in_specs=placed, out_specs=P(None, "seq"), check_vma=False
    )
```

```python
import jax
import jax.numpy as jnp
from jax import lax
from jax.experimental import pallas as pl
from jax.experimental.pallas import tpu as pltpu
from jax.sharding import PartitionSpec as P

MESH = pl.DeviceIdType.MESH
F32 = jnp.float32
BF16 = jnp.bfloat16

norm_epsilon = 1e-05
rope_base = 500000.0
masked_score = -1e30

NY, NZ, NH = 4, 16, 8
PLANE = [(dy, dh) for dy in range(NY) for dh in range(NH) if (dy, dh) != (0, 0)]
COLUMN = list(range(1, NZ))
WINDOW = [(dy, dz) for dy in (2, 1, 3) for dz in (2 if dy == 2 else -2, 1, -1, 0)]
WINDOW += [(0, 2), (0, 1), (0, -1)]
QUARTER = [6, -6, 2, -2]
HEADS = list(range(1, NH))
NEAR = [1, -1, 2, -2, 3, -3, 4, -4]
STAGES = 15


def kernel(
    hid_h, gain_h, wq_h, wk_h, wv_h, wo_h, down_h, up_h, choice_h, lengths_h, kc_h, vc_h,
    out,
    hid, gain, wq, wk, wv, wo, down, up, kc, vc, choice, lengths,
    t1a, t1b, flat, rsb_src, rsb, z2b, ups_src, ups, ups_y, z2e, agq, rso_src, rso, z2o, own_src, own_in, ago_src, ago, hbuf,
    load_sem, send_sem, recv_sem, vouch,
):
    seq = lax.axis_index("seq")
    head = lax.axis_index("head")
    core = lax.rem(head, 2)
    y = lax.rem(seq, NY)
    z = lax.div(seq, NY)
    mine = y * 4 + lax.rem(z, 4)
    first = y * 4 + lax.rem(z + 2, 4)

    def at(dy, dz, dh):
        yy = lax.rem(y + (dy + NY) % NY, NY)
        zz = lax.rem(z + (dz + NZ) % NZ, NZ)
        return (zz * NY + yy, lax.rem(head + (dh + NH) % NH, NH))

    loads = [
        pltpu.make_async_copy(src, dst, load_sem.at[k])
        for k, (src, dst) in enumerate(
            [(hid_h, hid), (gain_h, gain), (down_h, down), (wq_h, wq), (wk_h, wk), (wv_h, wv),
             (up_h, up), (kc_h, kc), (vc_h, vc), (wo_h, wo), (choice_h, choice),
             (lengths_h, lengths)]
        )
    ]
    for k in (10, 0, 1, 2, 6, 3, 4, 5, 7, 8, 9, 11):
        loads[k].start()

    barrier = pltpu.get_barrier_semaphore()
    greeted = [(0, dz, 0) for dz in NEAR]
    greeted += [(-dy, -dz, 0) for dy, dz in WINDOW if dy and dz]
    greeted += [(dy, 0, dh) for dy, dh in PLANE]
    for dy, dz, dh in greeted:
        pl.semaphore_signal(barrier, inc=1, device_id=at(dy, dz, dh), device_id_type=MESH)

    def send(stage, src, dst, where):
        pltpu.make_async_remote_copy(
            src_ref=src, dst_ref=dst, send_sem=send_sem.at[stage], recv_sem=recv_sem.at[stage],
            device_id=at(*where), device_id_type=MESH,
        ).start()

    def bundle(stage, view):
        return pltpu.make_async_remote_copy(
            src_ref=view, dst_ref=view, send_sem=send_sem.at[stage], recv_sem=recv_sem.at[stage],
            device_id=at(0, 1, 0), device_id_type=MESH,
        )

    rows = lax.broadcasted_iota(jnp.int32, (16, 128), 0)
    lane = lax.broadcasted_iota(jnp.int32, (16, 128), 1)
    group = lane // 16
    rows8 = lax.rem(rows, 8)
    lane8 = lax.broadcasted_iota(jnp.int32, (8, 128), 1)
    loads[10].wait()
    chosen = jnp.zeros((16, 128), jnp.int32)
    for r in range(16):
        chosen = jnp.where(rows == r, choice[r], chosen)

    for c in loads[:3]:
        c.wait()
    values = hid[...].astype(F32)
    scaled = (values * gain[...].astype(F32)).astype(BF16)
    every = lax.dot_general(
        scaled, down[...], (((1,), (1,)), ((), ())), preferred_element_type=F32
    )
    fold = jnp.zeros((16, 128), F32)
    for j in range(8):
        fold += jnp.where(
            chosen == head * 64 + j * 8 + group, every[:, j * 128 : (j + 1) * 128], 0.0
        )
    for shift in (64, 32, 16):
        fold += pltpu.roll(fold, shift, 1)
    diagonal = jnp.where(group == rows8, fold, 0.0)
    square = jnp.sum(values * values, axis=1, keepdims=True)
    t1a[0, 0:1, :] = jnp.sum(diagonal[0:8], axis=0, keepdims=True)
    t1a[0, 1:2, :] = jnp.sum(diagonal[8:16], axis=0, keepdims=True)

    loads[6].wait()
    for r in range(16):
        local = choice[r] - seq * 8
        found = up[jnp.clip(local, 0, 7)]
        here = (chosen[r : r + 1] >= seq * 8) & (chosen[r : r + 1] < seq * 8 + 8)
        here = jnp.broadcast_to(jnp.where(here, 1.0, 0.0), (16, 128)).astype(BF16)
        for j in range(8):
            ups_src[r % 4, r // 4, :, j * 128 : (j + 1) * 128] = found[:, j * 128 : (j + 1) * 128] * here

    for c in loads[3:6]:
        c.wait()
    query_part = jnp.dot(scaled, wq[...], preferred_element_type=F32)
    key_part = jnp.dot(scaled, wk[...], preferred_element_type=F32)
    value_part = jnp.dot(scaled, wv[...], preferred_element_type=F32)
    for j in range(8):
        flat[pl.ds(j, 16, stride=16), :] = query_part[:, j * 128 : (j + 1) * 128]
    flat[pl.ds(8, 16, stride=16), :] = key_part
    flat[pl.ds(9, 16, stride=16), :] = value_part
    flat[pl.ds(10, 16, stride=16), :] = jnp.broadcast_to(square, (16, 128))
    for j in range(11, 16):
        flat[pl.ds(j, 16, stride=16), :] = jnp.zeros((16, 128), F32)
    rsb_src[...] = flat[...].reshape(16, 16, 128).astype(BF16)

    pl.semaphore_wait(barrier, len(greeted))
    for k, (dy, dh) in enumerate(PLANE):
        send(0, t1a.at[0], t1a.at[k + 1], (dy, 0, dh))
    for dz in (4, -4):
        pl.semaphore_signal(vouch, inc=1, device_id=at(0, dz, 0), device_id_type=MESH)

    def row_of(dy, dz):
        return lax.rem(y + dy, 4) * 4 + lax.rem(z + dz + 6, 4)

    for k, (dy, dz) in enumerate(WINDOW):
        send(2, rsb_src.at[row_of(dy, dz)], rsb.at[k], (dy, dz, 0))
    for dz, k, low, high in ((2, 2, 0, 2), (-2, 2, 2, 4), (1, 0, 0, 4), (-1, 1, 0, 4)):
        part = ups_src.at[lax.rem(z + dz + 2, 4), low:high]
        send(4, part, ups.at[k, low:high], (0, dz, 0))

    bundle(0, t1a.at[1:32]).wait_recv()
    t1b[0] = jnp.sum(t1a[...], axis=0)
    pl.semaphore_wait(vouch, 2)
    for k, dz in enumerate(COLUMN):
        send(1, t1b.at[0], t1b.at[k + 1], (0, dz, 0))

    bundle(2, rsb).wait_recv()
    base = rsb_src[first].astype(F32)
    for k in range(15):
        base += rsb[k].astype(F32)
    z2b[0] = base.astype(BF16)
    for k, dz in enumerate(QUARTER):
        send(3, z2b.at[0], z2b.at[k + 1], (0, dz, 0))

    bundle(4, ups).wait_recv()
    ups_y[0] = (ups_src[lax.rem(z + 2, 4)] + ups[0]) + (ups[1] + ups[2])
    for dy in (2, 1, 3):
        send(11, ups_y.at[0, lax.rem(y + dy, 4)], ups_y.at[1, dy], (dy, 0, 0))

    loads[11].wait()
    half = lax.rem(lane8, 64).astype(F32)
    frequency = jnp.exp(-half * (jnp.log(jnp.full((8, 128), rope_base, F32)) / 64.0))
    angle = lengths[mine].astype(F32) * frequency
    cosine = jnp.cos(angle)
    sine = jnp.sin(angle)
    sine = jnp.where(lane8 < 64, -sine, sine)

    bundle(11, ups_y.at[1, 1:4]).wait_recv()
    up_rows = (ups_y[0, y] + ups_y[1, 1]) + (ups_y[1, 2] + ups_y[1, 3])
    bundle(1, t1b.at[1:16]).wait_recv()
    whole = jnp.sum(t1b[...], axis=0)
    ranks = jnp.where(first < 8, whole[0:1], whole[1:2])
    ranks = pltpu.roll(ranks, lax.rem(128 - 16 * lax.rem(first, 8), 128), 1)
    ranks = jnp.broadcast_to(ranks, (8, 128)).astype(BF16)
    expand = jnp.dot(ranks[:, 0:16], up_rows, preferred_element_type=F32)
    sub8 = lax.broadcasted_iota(jnp.int32, (8, 128), 0)
    grown = jnp.zeros((8, 128), F32)
    for j in range(8):
        grown += jnp.where(sub8 == j, expand[:, j * 128 : (j + 1) * 128], 0.0)
    z2e[0] = grown.astype(BF16)
    for k, dz in enumerate(QUARTER):
        send(5, z2e.at[0], z2e.at[k + 1], (0, dz, 0))

    bundle(3, z2b.at[1:5]).wait_recv()
    base = z2b[1].astype(F32)
    for k in range(2, 5):
        base += z2b[k].astype(F32)
    inverse = lax.rsqrt(base[10:11] * (1.0 / 8192.0) + norm_epsilon)

    def rotated(x):
        return (x * cosine + pltpu.roll(x, 64, 1) * sine).astype(BF16)

    key_rot = rotated(jnp.broadcast_to(base[8:9] * inverse, (8, 128))).astype(F32)
    value_own = jnp.broadcast_to(base[9:10] * inverse, (8, 128)).astype(BF16).astype(F32)
    bundle(5, z2e.at[1:5]).wait_recv()
    query = base[0:8]
    for k in range(1, 5):
        query += z2e[k].astype(F32)
    query_rot = rotated(query * inverse)
    agq[mine] = query_rot
    for dy, dz in WINDOW:
        send(6, agq.at[mine], agq.at[mine], (dy, dz, 0))
    scale = 128.0**-0.5
    own_score = jnp.sum(query_rot.astype(F32) * key_rot, axis=1, keepdims=True) * scale
    own_src[0:8, :] = jnp.broadcast_to(own_score, (8, 128))
    own_src[8:16, :] = value_own

    @pl.when(core == 0)
    def _():
        send(12, own_src, own_in, (0, 0, 1))

    def packed(high, low, total, result):
        stat = jnp.where(lane8 < 32, high, jnp.where(lane8 < 64, low, total))
        return jnp.concatenate([result, stat], axis=0).astype(BF16)

    def merged(parts):
        parts = [part.astype(F32) for part in parts]
        stats = [part[8:16] for part in parts]
        tops = [
            jnp.broadcast_to(stat[:, 0:1] + stat[:, 32:33], (8, 128)) for stat in stats
        ]
        totals = [jnp.broadcast_to(stat[:, 64:65], (8, 128)) for stat in stats]
        top = tops[0]
        for t in tops[1:]:
            top = jnp.maximum(top, t)
        high = top.astype(BF16).astype(F32)
        low = (top - high).astype(BF16).astype(F32)
        total = jnp.zeros((8, 128), F32)
        result = jnp.zeros((8, 128), F32)
        for t, s, part in zip(tops, totals, parts):
            factor = jnp.exp(t - (high + low))
            total += s * factor
            result += part[0:8] * factor
        return high, low, total, result

    loads[7].wait()
    loads[8].wait()
    bundle(6, agq.at[0:15]).wait_recv()
    position = lax.broadcasted_iota(jnp.int32, (8, 256), 1) + seq * 256
    each = range(16)
    scores = [
        lax.dot_general(agq[r], kc[r], (((1,), (1,)), ((), ())), preferred_element_type=F32)
        * scale
        for r in each
    ]
    valid = [position < lengths[r] for r in each]
    scores = [jnp.where(valid[r], scores[r], masked_score) for r in each]
    tops = [jnp.max(scores[r], axis=1, keepdims=True) for r in each]
    highs = [top.astype(BF16).astype(F32) for top in tops]
    lows = [(top - high).astype(BF16).astype(F32) for top, high in zip(tops, highs)]
    weights = [
        jnp.where(valid[r], jnp.exp(scores[r] - (highs[r] + lows[r])), 0.0) for r in each
    ]
    totals = [jnp.sum(weights[r], axis=1, keepdims=True) for r in each]
    results = [
        jnp.dot(weights[r].astype(BF16), vc[r], preferred_element_type=F32) for r in each
    ]
    for r in each:
        rso_src[r] = packed(highs[r], lows[r], totals[r], results[r])
    @pl.when(core == 0)
    def _():
        for k, (dy, dz) in enumerate(WINDOW):
            send(7, rso_src.at[row_of(dy, dz)], rso.at[k], (dy, dz, 1))
        send(7, rso_src.at[first], rso.at[15], (0, 0, 1))
        bundle(13, ago).wait_recv()

    @pl.when(core == 1)
    def _():
        for k, (dy, dz) in enumerate(WINDOW):
            send(14, rso_src.at[row_of(dy, dz)], rso.at[k + 16], (dy, dz, 0))

        bundle(7, rso.at[0:16]).wait_recv()
        z2o[0, 0] = packed(*merged([rso[k] for k in range(16)]))
        bundle(14, rso.at[16:31]).wait_recv()
        z2o[0, 1] = packed(*merged([rso_src[first]] + [rso[k] for k in range(16, 31)]))
        for k, dz in enumerate(QUARTER):
            send(8, z2o.at[0], z2o.at[k + 1], (0, dz, 0))

        def attended(slot, own_score, value_own):
            high, low, total, result = merged([z2o[k, slot] for k in range(1, 5)])
            top = high + low
            peak = jnp.maximum(top, own_score)
            factor = jnp.exp(top - peak)
            own_weight = jnp.exp(own_score - peak)
            summed = result * factor + own_weight * value_own
            return (summed / (total * factor + own_weight)).astype(BF16)

        bundle(12, own_in).wait_recv()
        bundle(8, z2o.at[1:5]).wait_recv()
        ago_src[...] = attended(0, own_in[0:8, :], own_in[8:16, :])
        ago[mine] = attended(1, own_src[0:8, :], own_src[8:16, :])
        for dy, dz in WINDOW:
            send(13, ago_src, ago.at[mine], (dy, dz, -1))
            send(9, ago.at[mine], ago.at[mine], (dy, dz, 0))
        send(13, ago_src, ago.at[mine], (0, 0, -1))
        bundle(9, ago.at[0:15]).wait_recv()

    loads[9].wait()
    flat[0:128, :] = ago[...].astype(F32).reshape(128, 128)
    projected = jnp.zeros((16, 128), F32)
    for j in range(8):
        projected += jnp.dot(
            flat[pl.ds(j, 16, stride=8), :].astype(BF16),
            wo[j * 128 : (j + 1) * 128, :],
            preferred_element_type=F32,
        )
    hbuf[0] = projected.astype(BF16)
    for k, dh in enumerate(HEADS):
        send(10, hbuf.at[0], hbuf.at[k + 1], (0, 0, dh))
    bundle(10, hbuf.at[1:8]).wait_recv()
    out[...] = jnp.sum(hbuf[...].astype(F32), axis=0).astype(BF16)

    sent = [
        (0, t1a.at[1:32]), (1, t1b.at[1:16]), (2, rsb), (3, z2b.at[1:5]), (4, ups),
        (5, z2e.at[1:5]), (6, agq.at[0:15]), (10, hbuf.at[1:8]), (11, ups_y.at[1, 1:4]),
    ]
    for stage, view in sent:
        bundle(stage, view).wait_send()

    @pl.when(core == 0)
    def _():
        bundle(12, own_in).wait_send()
        bundle(7, rso.at[0:16]).wait_send()

    @pl.when(core == 1)
    def _():
        bundle(14, rso.at[16:31]).wait_send()
        bundle(8, z2o.at[1:5]).wait_send()
        bundle(13, ago).wait_send()
        bundle(9, ago.at[0:15]).wait_send()


def body(hid, gain, wq, wk, wv, wo, down, up, choice, lengths, kc, vc):
    anywhere = pl.BlockSpec(memory_space=pl.ANY)
    return pl.pallas_call(
        kernel,
        out_shape=pltpu.VMEM((16, 128), BF16),
        in_specs=[anywhere] * 12,
        out_specs=pl.BlockSpec(memory_space=pltpu.VMEM),
        scratch_shapes=[
            pltpu.VMEM((16, 128), BF16),
            pltpu.VMEM((1, 128), BF16),
            pltpu.VMEM((128, 1024), BF16),
            pltpu.VMEM((128, 128), BF16),
            pltpu.VMEM((128, 128), BF16),
            pltpu.VMEM((1024, 128), BF16),
            pltpu.VMEM((1024, 128), BF16),
            pltpu.VMEM((8, 16, 1024), BF16),
            pltpu.VMEM((16, 256, 128), BF16),
            pltpu.VMEM((16, 256, 128), BF16),
            pltpu.SMEM((16,), jnp.int32),
            pltpu.SMEM((16,), jnp.int32),
            pltpu.VMEM((32, 2, 128), F32),
            pltpu.VMEM((16, 2, 128), F32),
            pltpu.VMEM((256, 128), F32),
            pltpu.VMEM((16, 16, 128), BF16),
            pltpu.VMEM((15, 16, 128), BF16),
            pltpu.VMEM((5, 16, 128), BF16),
            pltpu.VMEM((4, 4, 16, 1024), BF16),
            pltpu.VMEM((3, 4, 16, 1024), BF16),
            pltpu.VMEM((2, 4, 16, 1024), BF16),
            pltpu.VMEM((5, 8, 128), BF16),
            pltpu.VMEM((16, 8, 128), BF16),
            pltpu.VMEM((16, 16, 128), BF16),
            pltpu.VMEM((31, 16, 128), BF16),
            pltpu.VMEM((5, 2, 16, 128), BF16),
            pltpu.VMEM((16, 128), F32),
            pltpu.VMEM((16, 128), F32),
            pltpu.VMEM((8, 128), BF16),
            pltpu.VMEM((16, 8, 128), BF16),
            pltpu.VMEM((8, 16, 128), BF16),
            pltpu.SemaphoreType.DMA((12,)),
            pltpu.SemaphoreType.DMA((STAGES,)),
            pltpu.SemaphoreType.DMA((STAGES,)),
            pltpu.SemaphoreType.REGULAR,
        ],
        compiler_params=pltpu.CompilerParams(collective_id=0, has_side_effects=True),
    )(
        hid, gain.reshape(1, 128), wq, wk, wv, wo, down.reshape(1024, 128), up,
        choice, lengths, kc.reshape(16, 256, 128), vc.reshape(16, 256, 128),
    )


def solution(mesh):
    placed = (
        P(None, "seq"),
        P("seq"),
        P("seq", "head"),
        P("seq", "head"),
        P("seq", "head"),
        P("head", "seq"),
        P("head", None, "seq"),
        P("seq", None, "head"),
        P(),
        P(),
        P(None, "seq", "head", None),
        P(None, "seq", "head", None),
    )
    return jax.shard_map(
        body, mesh=mesh, in_specs=placed, out_specs=P(None, "seq"), check_vma=False
    )
```

```python
import jax
import jax.numpy as jnp
from jax import lax
from jax.experimental import pallas as pl
from jax.experimental.pallas import tpu as pltpu
from jax.sharding import PartitionSpec as P

MESH = pl.DeviceIdType.MESH
F32 = jnp.float32
BF16 = jnp.bfloat16

norm_epsilon = 1e-05
rope_base = 500000.0
masked_score = -1e30

NY, NZ, NH = 4, 16, 8
PLANE = [(dy, dh) for dy in (2, 1, 3, 0) for dh in range(NH) if (dy, dh) != (0, 0)]
COLUMN = list(range(1, NZ))
WINDOW = [(dy, dz) for dy in (2, 1, 3) for dz in (2 if dy == 2 else -2, 1, -1, 0)]
WINDOW += [(0, 2), (0, 1), (0, -1)]
QUARTER = [6, -6, 2, -2]
HEADS = list(range(1, NH))
NEAR = [1, -1, 2, -2, 3, -3, 4, -4]
STAGES = 18


def kernel(
    hid_h, gain_h, wq_h, wk_h, wv_h, wo_h, down_h, up_h, choice_h, lengths_h, kc_h, vc_h,
    out,
    hid, gain, wq, wk, wv, wo, down, up, kc, vc, choice, lengths,
    t1_src, t1a, t1b, flat, rsb_src, rsb, z2b, ups_src, ups, ups_y, ups_in, z2e, agq_src, agq, rso_src, rso, z2o, own_src, own_in, own, ago_src, ago, hbuf,
    load_sem, send_sem, recv_sem, vouch,
):
    seq = lax.axis_index("seq")
    head = lax.axis_index("head")
    core = lax.rem(head, 2)
    y = lax.rem(seq, NY)
    z = lax.div(seq, NY)
    mine = y * 4 + lax.rem(z, 4)
    first = y * 4 + lax.rem(z + 2, 4)

    def at(dy, dz, dh):
        yy = lax.rem(y + (dy + NY) % NY, NY)
        zz = lax.rem(z + (dz + NZ) % NZ, NZ)
        return (zz * NY + yy, lax.rem(head + dh + NH, NH))

    loads = [
        pltpu.make_async_copy(src, dst, load_sem.at[k])
        for k, (src, dst) in enumerate(
            [(hid_h, hid), (gain_h, gain), (down_h, down), (wq_h, wq), (wk_h, wk), (wv_h, wv),
             (up_h, up), (kc_h, kc), (vc_h, vc), (wo_h, wo), (choice_h, choice),
             (lengths_h, lengths)]
        )
    ]
    for k in (10, 0, 1, 2, 6, 3, 4, 5, 7, 8, 9, 11):
        loads[k].start()

    barrier = pltpu.get_barrier_semaphore()
    greeted = [(dy, 0, dh) for dy, dh in PLANE]
    greeted += [(0, dz, 0) for dz in NEAR]
    greeted += [(-dy, -dz, 0) for dy, dz in WINDOW if dy and dz]
    for dy, dz, dh in greeted:
        pl.semaphore_signal(barrier, inc=1, device_id=at(dy, dz, dh), device_id_type=MESH)

    def send(stage, src, dst, where):
        pltpu.make_async_remote_copy(
            src_ref=src, dst_ref=dst, send_sem=send_sem.at[stage], recv_sem=recv_sem.at[stage],
            device_id=at(*where), device_id_type=MESH,
        ).start()

    def bundle(stage, view):
        return pltpu.make_async_remote_copy(
            src_ref=view, dst_ref=view, send_sem=send_sem.at[stage], recv_sem=recv_sem.at[stage],
            device_id=at(0, 1, 0), device_id_type=MESH,
        )

    rows = lax.broadcasted_iota(jnp.int32, (16, 128), 0)
    lane = lax.broadcasted_iota(jnp.int32, (16, 128), 1)
    group = lane // 16
    rows8 = lax.rem(rows, 8)
    lane8 = lax.broadcasted_iota(jnp.int32, (8, 128), 1)
    loads[10].wait()
    chosen = jnp.zeros((16, 128), jnp.int32)
    for r in range(16):
        chosen = jnp.where(rows == r, choice[r], chosen)

    for c in loads[:3]:
        c.wait()
    values = hid[...].astype(F32)
    scaled = (values * gain[...].astype(F32)).astype(BF16)
    every = lax.dot_general(
        scaled, down[...], (((1,), (1,)), ((), ())), preferred_element_type=F32
    )
    fold = jnp.zeros((16, 128), F32)
    for j in range(8):
        fold += jnp.where(
            chosen == head * 64 + j * 8 + group, every[:, j * 128 : (j + 1) * 128], 0.0
        )
    for shift in (64, 32, 16):
        fold += pltpu.roll(fold, shift, 1)
    diagonal = jnp.where(group == rows8, fold, 0.0)
    square = jnp.sum(values * values, axis=1, keepdims=True)
    t1_src[0:1, :] = jnp.sum(diagonal[0:8], axis=0, keepdims=True)
    t1_src[1:2, :] = jnp.sum(diagonal[8:16], axis=0, keepdims=True)

    loads[6].wait()
    for r in range(16):
        local = choice[r] - seq * 8
        found = up[jnp.clip(local, 0, 7)]
        here = (chosen[r : r + 1] >= seq * 8) & (chosen[r : r + 1] < seq * 8 + 8)
        here = jnp.broadcast_to(jnp.where(here, 1.0, 0.0), (16, 128)).astype(BF16)
        for j in range(8):
            ups_src[r % 4, r // 4, :, j * 128 : (j + 1) * 128] = found[:, j * 128 : (j + 1) * 128] * here

    for c in loads[3:6]:
        c.wait()
    query_part = jnp.dot(scaled, wq[...], preferred_element_type=F32)
    key_part = jnp.dot(scaled, wk[...], preferred_element_type=F32)
    value_part = jnp.dot(scaled, wv[...], preferred_element_type=F32)
    for j in range(8):
        flat[pl.ds(j, 16, stride=16), :] = query_part[:, j * 128 : (j + 1) * 128]
    flat[pl.ds(8, 16, stride=16), :] = key_part
    flat[pl.ds(9, 16, stride=16), :] = value_part
    flat[pl.ds(10, 16, stride=16), :] = jnp.broadcast_to(square, (16, 128))
    for j in range(11, 16):
        flat[pl.ds(j, 16, stride=16), :] = jnp.zeros((16, 128), F32)
    rsb_src[...] = flat[...].reshape(16, 16, 128).astype(BF16)

    pl.semaphore_wait(barrier, len(greeted))
    for dy in (2, 1, 3, 0):
        for dx in (2, 1, 3, 0):
            if (dy, dx) != (0, 0):
                send(0, t1_src, t1a.at[(dy * 4 + dx) * 2 + core], (dy, 0, 2 * dx + 1 - core))

    @pl.when(core == 0)
    def _():
        send(17, t1_src, t1a.at[0], (0, 0, 1))

    @pl.when(core == 1)
    def _():
        t1a[1] = t1_src[...]
    for dz in (4, -4):
        pl.semaphore_signal(vouch, inc=1, device_id=at(0, dz, 0), device_id_type=MESH)

    def row_of(dy, dz):
        return lax.rem(y + dy, 4) * 4 + lax.rem(z + dz + 6, 4)

    for k, (dy, dz) in enumerate(WINDOW):
        send(2, rsb_src.at[row_of(dy, dz)], rsb.at[k], (dy, dz, 0))
    for dz, k, low, high in ((2, 2, 0, 2), (-2, 2, 2, 4), (1, 0, 0, 4), (-1, 1, 0, 4)):
        part = ups_src.at[lax.rem(z + dz + 2, 4), low:high]
        send(4, part, ups.at[k, low:high], (0, dz, 0))

    pl.semaphore_wait(vouch, 2)

    @pl.when(core == 1)
    def _():
        bundle(0, t1a.at[2:32]).wait_recv()
        bundle(17, t1a.at[0]).wait_recv()
        t1b[0] = jnp.sum(t1a[...], axis=0)
        for k, dz in enumerate(COLUMN):
            send(1, t1b.at[0], t1b.at[k + 1], (0, dz, 0))

    bundle(2, rsb).wait_recv()
    base = rsb_src[first].astype(F32)
    for k in range(15):
        base += rsb[k].astype(F32)
    z2b[0] = base.astype(BF16)
    for k, dz in enumerate(QUARTER):
        send(3, z2b.at[0], z2b.at[k + 1], (0, dz, 0))

    bundle(4, ups).wait_recv()
    ups_y[...] = (ups_src[lax.rem(z + 2, 4)] + ups[0]) + (ups[1] + ups[2])

    @pl.when(core == 0)
    def _():
        for k, dy in enumerate((2, 1, 3)):
            send(15, ups_y.at[lax.rem(y + dy, 4)], ups_in.at[k], (dy, 0, 1))
        send(15, ups_y.at[y], ups_in.at[3], (0, 0, 1))

    @pl.when(core == 1)
    def _():
        for k, dy in enumerate((2, 1, 3)):
            send(11, ups_y.at[lax.rem(y + dy, 4)], ups_in.at[k + 4], (dy, 0, 0))

    loads[11].wait()
    half = lax.rem(lane8, 64).astype(F32)
    frequency = jnp.exp(-half * (jnp.log(jnp.full((8, 128), rope_base, F32)) / 64.0))
    angle = lengths[mine].astype(F32) * frequency
    cosine = jnp.cos(angle)
    sine = jnp.sin(angle)
    sine = jnp.where(lane8 < 64, -sine, sine)

    def rotated(x):
        return (x * cosine + pltpu.roll(x, 64, 1) * sine).astype(BF16)

    def sum_base():
        bundle(3, z2b.at[1:5]).wait_recv()
        base = z2b[1].astype(F32)
        for k in range(2, 5):
            base += z2b[k].astype(F32)
        own_src[...] = base

    scale = 128.0**-0.5

    @pl.when(core == 0)
    def _():
        sum_base()
        send(12, own_src, own_in, (0, 0, 1))
        bundle(16, agq).wait_recv()

    @pl.when(core == 1)
    def _():
        bundle(11, ups_in.at[4:7]).wait_recv()
        bundle(15, ups_in.at[0:4]).wait_recv()
        up_even = (ups_in[0] + ups_in[1]) + (ups_in[2] + ups_in[3])
        up_odd = (ups_y[y] + ups_in[4]) + (ups_in[5] + ups_in[6])
        bundle(1, t1b.at[1:16]).wait_recv()
        whole = jnp.sum(t1b[...], axis=0)
        ranks = jnp.where(first < 8, whole[0:1], whole[1:2])
        ranks = pltpu.roll(ranks, lax.rem(128 - 16 * lax.rem(first, 8), 128), 1)
        ranks = jnp.broadcast_to(ranks, (8, 128)).astype(BF16)
        sub8 = lax.broadcasted_iota(jnp.int32, (8, 128), 0)
        for slot, up_rows in enumerate((up_even, up_odd)):
            expand = jnp.dot(ranks[:, 0:16], up_rows, preferred_element_type=F32)
            grown = jnp.zeros((8, 128), F32)
            for j in range(8):
                grown += jnp.where(sub8 == j, expand[:, j * 128 : (j + 1) * 128], 0.0)
            z2e[0, slot] = grown.astype(BF16)
        for k, dz in enumerate(QUARTER):
            send(5, z2e.at[0], z2e.at[k + 1], (0, dz, 0))

        sum_base()
        bundle(12, own_in).wait_recv()
        bases = (own_in[...], own_src[...])
        inverses = [lax.rsqrt(base[10:11] * (1.0 / 8192.0) + norm_epsilon) for base in bases]
        bundle(5, z2e.at[1:5]).wait_recv()
        queries = []
        for slot, (base, inverse) in enumerate(zip(bases, inverses)):
            query = base[0:8]
            for k in range(1, 5):
                query += z2e[k, slot].astype(F32)
            queries.append(rotated(query * inverse))
        agq_src[...] = queries[0]
        agq[mine] = queries[1]
        for dy, dz in WINDOW:
            send(16, agq_src, agq.at[mine], (dy, dz, -1))
            send(6, agq.at[mine], agq.at[mine], (dy, dz, 0))
        send(16, agq_src, agq.at[mine], (0, 0, -1))
        for slot, (base, inverse) in enumerate(zip(bases, inverses)):
            key_rot = rotated(jnp.broadcast_to(base[8:9] * inverse, (8, 128))).astype(F32)
            value_own = jnp.broadcast_to(base[9:10] * inverse, (8, 128)).astype(BF16)
            own_score = jnp.sum(queries[slot].astype(F32) * key_rot, axis=1, keepdims=True)
            own[slot, 0:8, :] = jnp.broadcast_to(own_score * scale, (8, 128))
            own[slot, 8:16, :] = value_own.astype(F32)
        bundle(6, agq.at[0:15]).wait_recv()

    def packed(high, low, total, result):
        stat = jnp.where(lane8 < 32, high, jnp.where(lane8 < 64, low, total))
        return jnp.concatenate([result, stat], axis=0).astype(BF16)

    def merged(parts):
        parts = [part.astype(F32) for part in parts]
        stats = [part[8:16] for part in parts]
        tops = [
            jnp.broadcast_to(stat[:, 0:1] + stat[:, 32:33], (8, 128)) for stat in stats
        ]
        totals = [jnp.broadcast_to(stat[:, 64:65], (8, 128)) for stat in stats]
        top = tops[0]
        for t in tops[1:]:
            top = jnp.maximum(top, t)
        high = top.astype(BF16).astype(F32)
        low = (top - high).astype(BF16).astype(F32)
        total = jnp.zeros((8, 128), F32)
        result = jnp.zeros((8, 128), F32)
        for t, s, part in zip(tops, totals, parts):
            factor = jnp.exp(t - (high + low))
            total += s * factor
            result += part[0:8] * factor
        return high, low, total, result

    loads[7].wait()
    loads[8].wait()
    position = lax.broadcasted_iota(jnp.int32, (8, 256), 1) + seq * 256
    each = range(16)
    scores = [
        lax.dot_general(agq[r], kc[r], (((1,), (1,)), ((), ())), preferred_element_type=F32)
        * scale
        for r in each
    ]
    valid = [position < lengths[r] for r in each]
    scores = [jnp.where(valid[r], scores[r], masked_score) for r in each]
    tops = [jnp.max(scores[r], axis=1, keepdims=True) for r in each]
    highs = [top.astype(BF16).astype(F32) for top in tops]
    lows = [(top - high).astype(BF16).astype(F32) for top, high in zip(tops, highs)]
    weights = [
        jnp.where(valid[r], jnp.exp(scores[r] - (highs[r] + lows[r])), 0.0) for r in each
    ]
    totals = [jnp.sum(weights[r], axis=1, keepdims=True) for r in each]
    results = [
        jnp.dot(weights[r].astype(BF16), vc[r], preferred_element_type=F32) for r in each
    ]
    for r in each:
        rso_src[r] = packed(highs[r], lows[r], totals[r], results[r])
    @pl.when(core == 0)
    def _():
        for k, (dy, dz) in enumerate(WINDOW):
            send(7, rso_src.at[row_of(dy, dz)], rso.at[k], (dy, dz, 1))
        send(7, rso_src.at[first], rso.at[15], (0, 0, 1))
        bundle(13, ago).wait_recv()

    @pl.when(core == 1)
    def _():
        for k, (dy, dz) in enumerate(WINDOW):
            send(14, rso_src.at[row_of(dy, dz)], rso.at[k + 16], (dy, dz, 0))

        bundle(7, rso.at[0:16]).wait_recv()
        z2o[0, 0] = packed(*merged([rso[k] for k in range(16)]))
        bundle(14, rso.at[16:31]).wait_recv()
        z2o[0, 1] = packed(*merged([rso_src[first]] + [rso[k] for k in range(16, 31)]))
        for k, dz in enumerate(QUARTER):
            send(8, z2o.at[0], z2o.at[k + 1], (0, dz, 0))

        def attended(slot, own_score, value_own):
            high, low, total, result = merged([z2o[k, slot] for k in range(1, 5)])
            top = high + low
            peak = jnp.maximum(top, own_score)
            factor = jnp.exp(top - peak)
            own_weight = jnp.exp(own_score - peak)
            summed = result * factor + own_weight * value_own
            return (summed / (total * factor + own_weight)).astype(BF16)

        bundle(8, z2o.at[1:5]).wait_recv()
        ago_src[...] = attended(0, own[0, 0:8, :], own[0, 8:16, :])
        ago[mine] = attended(1, own[1, 0:8, :], own[1, 8:16, :])
        for dy, dz in WINDOW:
            send(13, ago_src, ago.at[mine], (dy, dz, -1))
            send(9, ago.at[mine], ago.at[mine], (dy, dz, 0))
        send(13, ago_src, ago.at[mine], (0, 0, -1))
        bundle(9, ago.at[0:15]).wait_recv()

    loads[9].wait()
    flat[0:128, :] = ago[...].astype(F32).reshape(128, 128)
    projected = jnp.zeros((16, 128), F32)
    for j in range(8):
        projected += jnp.dot(
            flat[pl.ds(j, 16, stride=8), :].astype(BF16),
            wo[j * 128 : (j + 1) * 128, :],
            preferred_element_type=F32,
        )
    hbuf[0] = projected.astype(BF16)
    for k, dh in enumerate(HEADS):
        send(10, hbuf.at[0], hbuf.at[k + 1], (0, 0, dh))
    bundle(10, hbuf.at[1:8]).wait_recv()
    out[...] = jnp.sum(hbuf[...].astype(F32), axis=0).astype(BF16)

    sent = [
        (0, t1a.at[0:15]), (2, rsb), (3, z2b.at[1:5]), (4, ups), (10, hbuf.at[1:8]),
    ]
    for stage, view in sent:
        bundle(stage, view).wait_send()

    @pl.when(core == 0)
    def _():
        bundle(17, t1_src).wait_send()
        bundle(12, own_in).wait_send()
        bundle(15, ups_in.at[0:4]).wait_send()
        bundle(7, rso.at[0:16]).wait_send()

    @pl.when(core == 1)
    def _():
        bundle(1, t1b.at[1:16]).wait_send()
        bundle(11, ups_in.at[4:7]).wait_send()
        bundle(5, z2e.at[1:5]).wait_send()
        bundle(16, agq).wait_send()
        bundle(6, agq.at[0:15]).wait_send()
        bundle(14, rso.at[16:31]).wait_send()
        bundle(8, z2o.at[1:5]).wait_send()
        bundle(13, ago).wait_send()
        bundle(9, ago.at[0:15]).wait_send()


def body(hid, gain, wq, wk, wv, wo, down, up, choice, lengths, kc, vc):
    anywhere = pl.BlockSpec(memory_space=pl.ANY)
    return pl.pallas_call(
        kernel,
        out_shape=pltpu.VMEM((16, 128), BF16),
        in_specs=[anywhere] * 12,
        out_specs=pl.BlockSpec(memory_space=pltpu.VMEM),
        scratch_shapes=[
            pltpu.VMEM((16, 128), BF16),
            pltpu.VMEM((1, 128), BF16),
            pltpu.VMEM((128, 1024), BF16),
            pltpu.VMEM((128, 128), BF16),
            pltpu.VMEM((128, 128), BF16),
            pltpu.VMEM((1024, 128), BF16),
            pltpu.VMEM((1024, 128), BF16),
            pltpu.VMEM((8, 16, 1024), BF16),
            pltpu.VMEM((16, 256, 128), BF16),
            pltpu.VMEM((16, 256, 128), BF16),
            pltpu.SMEM((16,), jnp.int32),
            pltpu.SMEM((16,), jnp.int32),
            pltpu.VMEM((2, 128), F32),
            pltpu.VMEM((32, 2, 128), F32),
            pltpu.VMEM((16, 2, 128), F32),
            pltpu.VMEM((256, 128), F32),
            pltpu.VMEM((16, 16, 128), BF16),
            pltpu.VMEM((15, 16, 128), BF16),
            pltpu.VMEM((5, 16, 128), BF16),
            pltpu.VMEM((4, 4, 16, 1024), BF16),
            pltpu.VMEM((3, 4, 16, 1024), BF16),
            pltpu.VMEM((4, 16, 1024), BF16),
            pltpu.VMEM((7, 16, 1024), BF16),
            pltpu.VMEM((5, 2, 8, 128), BF16),
            pltpu.VMEM((8, 128), BF16),
            pltpu.VMEM((16, 8, 128), BF16),
            pltpu.VMEM((16, 16, 128), BF16),
            pltpu.VMEM((31, 16, 128), BF16),
            pltpu.VMEM((5, 2, 16, 128), BF16),
            pltpu.VMEM((16, 128), F32),
            pltpu.VMEM((16, 128), F32),
            pltpu.VMEM((2, 16, 128), F32),
            pltpu.VMEM((8, 128), BF16),
            pltpu.VMEM((16, 8, 128), BF16),
            pltpu.VMEM((8, 16, 128), BF16),
            pltpu.SemaphoreType.DMA((12,)),
            pltpu.SemaphoreType.DMA((STAGES,)),
            pltpu.SemaphoreType.DMA((STAGES,)),
            pltpu.SemaphoreType.REGULAR,
        ],
        compiler_params=pltpu.CompilerParams(collective_id=0, has_side_effects=True),
    )(
        hid, gain.reshape(1, 128), wq, wk, wv, wo, down.reshape(1024, 128), up,
        choice, lengths, kc.reshape(16, 256, 128), vc.reshape(16, 256, 128),
    )


def solution(mesh):
    placed = (
        P(None, "seq"),
        P("seq"),
        P("seq", "head"),
        P("seq", "head"),
        P("seq", "head"),
        P("head", "seq"),
        P("head", None, "seq"),
        P("seq", None, "head"),
        P(),
        P(),
        P(None, "seq", "head", None),
        P(None, "seq", "head", None),
    )
    return jax.shard_map(
        body, mesh=mesh, in_specs=placed, out_specs=P(None, "seq"), check_vma=False
    )
```

```python
import jax
import jax.numpy as jnp
from jax import lax
from jax.experimental import pallas as pl
from jax.experimental.pallas import tpu as pltpu
from jax.sharding import PartitionSpec as P

MESH = pl.DeviceIdType.MESH
F32 = jnp.float32
BF16 = jnp.bfloat16

norm_epsilon = 1e-05
rope_base = 500000.0
masked_score = -1e30

NY, NZ, NH = 4, 16, 8
PLANE = [(dy, dh) for dy in (2, 1, 3, 0) for dh in range(NH) if (dy, dh) != (0, 0)]
COLUMN = list(range(1, NZ))
WINDOW = [(dy, dz) for dy in (2, 1, 3) for dz in (2 if dy == 2 else -2, 1, -1, 0)]
WINDOW += [(0, 2), (0, 1), (0, -1)]
QUARTER = [6, -6, 2, -2]
HEADS = list(range(1, NH))
NEAR = [1, -1, 2, -2, 3, -3, 4, -4]
STAGES = 18


def kernel(
    hid_h, gain_h, wq_h, wk_h, wv_h, wo_h, down_h, up_h, choice_h, lengths_h, kc_h, vc_h,
    out,
    hid, gain, wq, wk, wv, wo, down, up, kc, vc, choice, lengths,
    t1_src, t1a, t1b, flat, rsb_src, rsb, z2b, ups_src, ups, ups_y, ups_in, z2e, agq_src, agq, rso_src, rso, z2o, own_src, own_in, own, ago_src, ago, hbuf,
    load_sem, send_sem, recv_sem, vouch,
):
    seq = lax.axis_index("seq")
    head = lax.axis_index("head")
    core = lax.rem(head, 2)
    y = lax.rem(seq, NY)
    z = lax.div(seq, NY)
    mine = y * 4 + lax.rem(z, 4)
    first = y * 4 + lax.rem(z + 2, 4)

    def at(dy, dz, dh):
        yy = lax.rem(y + (dy + NY) % NY, NY)
        zz = lax.rem(z + (dz + NZ) % NZ, NZ)
        return (zz * NY + yy, lax.rem(head + dh + NH, NH))

    loads = [
        pltpu.make_async_copy(src, dst, load_sem.at[k])
        for k, (src, dst) in enumerate(
            [(hid_h, hid), (gain_h, gain), (down_h, down), (wq_h, wq), (wk_h, wk), (wv_h, wv),
             (up_h, up), (kc_h, kc), (vc_h, vc), (wo_h, wo), (choice_h, choice),
             (lengths_h, lengths)]
        )
    ]
    for k in (10, 0, 1, 2, 6, 3, 4, 5, 7, 8, 9, 11):
        loads[k].start()

    barrier = pltpu.get_barrier_semaphore()
    greeted = [(dy, 0, dh) for dy, dh in PLANE]
    greeted += [(0, dz, 0) for dz in NEAR]
    greeted += [(-dy, -dz, 0) for dy, dz in WINDOW if dy and dz]
    for dy, dz, dh in greeted:
        pl.semaphore_signal(barrier, inc=1, device_id=at(dy, dz, dh), device_id_type=MESH)

    def send(stage, src, dst, where):
        pltpu.make_async_remote_copy(
            src_ref=src, dst_ref=dst, send_sem=send_sem.at[stage], recv_sem=recv_sem.at[stage],
            device_id=at(*where), device_id_type=MESH,
        ).start()

    def bundle(stage, view):
        return pltpu.make_async_remote_copy(
            src_ref=view, dst_ref=view, send_sem=send_sem.at[stage], recv_sem=recv_sem.at[stage],
            device_id=at(0, 1, 0), device_id_type=MESH,
        )

    rows = lax.broadcasted_iota(jnp.int32, (16, 128), 0)
    lane = lax.broadcasted_iota(jnp.int32, (16, 128), 1)
    group = lane // 16
    rows8 = lax.rem(rows, 8)
    lane8 = lax.broadcasted_iota(jnp.int32, (8, 128), 1)
    loads[10].wait()
    chosen = jnp.zeros((16, 128), jnp.int32)
    for r in range(16):
        chosen = jnp.where(rows == r, choice[r], chosen)

    for c in loads[:3]:
        c.wait()
    values = hid[...].astype(F32)
    scaled = (values * gain[...].astype(F32)).astype(BF16)
    every = lax.dot_general(
        scaled, down[...], (((1,), (1,)), ((), ())), preferred_element_type=F32
    )
    fold = jnp.zeros((16, 128), F32)
    for j in range(8):
        fold += jnp.where(
            chosen == head * 64 + j * 8 + group, every[:, j * 128 : (j + 1) * 128], 0.0
        )
    for shift in (64, 32, 16):
        fold += pltpu.roll(fold, shift, 1)
    diagonal = jnp.where(group == rows8, fold, 0.0)
    square = jnp.sum(values * values, axis=1, keepdims=True)
    t1_src[0:1, :] = jnp.sum(diagonal[0:8], axis=0, keepdims=True)
    t1_src[1:2, :] = jnp.sum(diagonal[8:16], axis=0, keepdims=True)

    loads[6].wait()
    for r in range(16):
        local = choice[r] - seq * 8
        found = up[jnp.clip(local, 0, 7)]
        here = (chosen[r : r + 1] >= seq * 8) & (chosen[r : r + 1] < seq * 8 + 8)
        here = jnp.broadcast_to(jnp.where(here, 1.0, 0.0), (16, 128)).astype(BF16)
        for j in range(8):
            ups_src[r % 4, r // 4, :, j * 128 : (j + 1) * 128] = found[:, j * 128 : (j + 1) * 128] * here

    for c in loads[3:6]:
        c.wait()
    query_part = jnp.dot(scaled, wq[...], preferred_element_type=F32)
    key_part = jnp.dot(scaled, wk[...], preferred_element_type=F32)
    value_part = jnp.dot(scaled, wv[...], preferred_element_type=F32)
    for j in range(8):
        flat[pl.ds(j, 16, stride=16), :] = query_part[:, j * 128 : (j + 1) * 128]
    flat[pl.ds(8, 16, stride=16), :] = key_part
    flat[pl.ds(9, 16, stride=16), :] = value_part
    flat[pl.ds(10, 16, stride=16), :] = jnp.broadcast_to(square, (16, 128))
    for j in range(11, 16):
        flat[pl.ds(j, 16, stride=16), :] = jnp.zeros((16, 128), F32)
    rsb_src[...] = flat[...].reshape(16, 16, 128).astype(BF16)

    pl.semaphore_wait(barrier, len(greeted))
    for dy in (2, 1, 3, 0):
        for dx in (2, 1, 3, 0):
            if (dy, dx) != (0, 0):
                send(0, t1_src, t1a.at[(dy * 4 + dx) * 2 + core], (dy, 0, 2 * dx + 1 - core))

    @pl.when(core == 0)
    def _():
        send(17, t1_src, t1a.at[0], (0, 0, 1))

    @pl.when(core == 1)
    def _():
        t1a[1] = t1_src[...]
    for dz in (4, -4):
        pl.semaphore_signal(vouch, inc=1, device_id=at(0, dz, 0), device_id_type=MESH)

    def row_of(dy, dz):
        return lax.rem(y + dy, 4) * 4 + lax.rem(z + dz + 6, 4)

    for dz, k, low, high in ((2, 2, 0, 2), (-2, 2, 2, 4), (1, 0, 0, 4), (-1, 1, 0, 4)):
        part = ups_src.at[lax.rem(z + dz + 2, 4), low:high]
        send(4, part, ups.at[k, low:high], (0, dz, 0))
    for k, (dy, dz) in enumerate(WINDOW):
        send(2, rsb_src.at[row_of(dy, dz)], rsb.at[k], (dy, dz, 0))

    pl.semaphore_wait(vouch, 2)

    @pl.when(core == 1)
    def _():
        bundle(0, t1a.at[2:32]).wait_recv()
        bundle(17, t1a.at[0]).wait_recv()
        t1b[0] = jnp.sum(t1a[...], axis=0)
        for k, dz in enumerate(COLUMN):
            send(1, t1b.at[0], t1b.at[k + 1], (0, dz, 0))

    bundle(2, rsb).wait_recv()
    base = rsb_src[first].astype(F32)
    for k in range(15):
        base += rsb[k].astype(F32)
    z2b[0] = base.astype(BF16)
    for k, dz in enumerate(QUARTER):
        send(3, z2b.at[0], z2b.at[k + 1], (0, dz, 0))

    bundle(4, ups).wait_recv()
    ups_y[...] = (ups_src[lax.rem(z + 2, 4)] + ups[0]) + (ups[1] + ups[2])

    @pl.when(core == 0)
    def _():
        for k, dy in enumerate((2, 1, 3)):
            send(15, ups_y.at[lax.rem(y + dy, 4)], ups_in.at[k], (dy, 0, 1))
        send(15, ups_y.at[y], ups_in.at[3], (0, 0, 1))

    @pl.when(core == 1)
    def _():
        for k, dy in enumerate((2, 1, 3)):
            send(11, ups_y.at[lax.rem(y + dy, 4)], ups_in.at[k + 4], (dy, 0, 0))

    loads[11].wait()
    half = lax.rem(lane8, 64).astype(F32)
    frequency = jnp.exp(-half * (jnp.log(jnp.full((8, 128), rope_base, F32)) / 64.0))
    angle = lengths[mine].astype(F32) * frequency
    cosine = jnp.cos(angle)
    sine = jnp.sin(angle)
    sine = jnp.where(lane8 < 64, -sine, sine)

    def rotated(x):
        return (x * cosine + pltpu.roll(x, 64, 1) * sine).astype(BF16)

    def sum_base():
        bundle(3, z2b.at[1:5]).wait_recv()
        base = z2b[1].astype(F32)
        for k in range(2, 5):
            base += z2b[k].astype(F32)
        own_src[...] = base

    scale = 128.0**-0.5

    @pl.when(core == 0)
    def _():
        sum_base()
        send(12, own_src, own_in, (0, 0, 1))
        bundle(16, agq).wait_recv()

    @pl.when(core == 1)
    def _():
        bundle(11, ups_in.at[4:7]).wait_recv()
        bundle(15, ups_in.at[0:4]).wait_recv()
        up_even = (ups_in[0] + ups_in[1]) + (ups_in[2] + ups_in[3])
        up_odd = (ups_y[y] + ups_in[4]) + (ups_in[5] + ups_in[6])
        bundle(1, t1b.at[1:16]).wait_recv()
        whole = jnp.sum(t1b[...], axis=0)
        ranks = jnp.where(first < 8, whole[0:1], whole[1:2])
        ranks = pltpu.roll(ranks, lax.rem(128 - 16 * lax.rem(first, 8), 128), 1)
        ranks = jnp.broadcast_to(ranks, (8, 128)).astype(BF16)
        sub8 = lax.broadcasted_iota(jnp.int32, (8, 128), 0)
        for slot, up_rows in enumerate((up_even, up_odd)):
            expand = jnp.dot(ranks[:, 0:16], up_rows, preferred_element_type=F32)
            grown = jnp.zeros((8, 128), F32)
            for j in range(8):
                grown += jnp.where(sub8 == j, expand[:, j * 128 : (j + 1) * 128], 0.0)
            z2e[0, slot] = grown.astype(BF16)
        for k, dz in enumerate(QUARTER):
            send(5, z2e.at[0], z2e.at[k + 1], (0, dz, 0))

        sum_base()
        bundle(12, own_in).wait_recv()
        bases = (own_in[...], own_src[...])
        inverses = [lax.rsqrt(base[10:11] * (1.0 / 8192.0) + norm_epsilon) for base in bases]
        bundle(5, z2e.at[1:5]).wait_recv()
        queries = []
        for slot, (base, inverse) in enumerate(zip(bases, inverses)):
            query = base[0:8]
            for k in range(1, 5):
                query += z2e[k, slot].astype(F32)
            queries.append(rotated(query * inverse))
        agq_src[...] = queries[0]
        agq[mine] = queries[1]
        for dy, dz in WINDOW:
            send(16, agq_src, agq.at[mine], (dy, dz, -1))
            send(6, agq.at[mine], agq.at[mine], (dy, dz, 0))
        send(16, agq_src, agq.at[mine], (0, 0, -1))
        for slot, (base, inverse) in enumerate(zip(bases, inverses)):
            key_rot = rotated(jnp.broadcast_to(base[8:9] * inverse, (8, 128))).astype(F32)
            value_own = jnp.broadcast_to(base[9:10] * inverse, (8, 128)).astype(BF16)
            own_score = jnp.sum(queries[slot].astype(F32) * key_rot, axis=1, keepdims=True)
            own[slot, 0:8, :] = jnp.broadcast_to(own_score * scale, (8, 128))
            own[slot, 8:16, :] = value_own.astype(F32)
        bundle(6, agq.at[0:15]).wait_recv()

    def packed(high, low, total, result):
        stat = jnp.where(lane8 < 32, high, jnp.where(lane8 < 64, low, total))
        return jnp.concatenate([result, stat], axis=0).astype(BF16)

    def merged(parts):
        parts = [part.astype(F32) for part in parts]
        stats = [part[8:16] for part in parts]
        tops = [
            jnp.broadcast_to(stat[:, 0:1] + stat[:, 32:33], (8, 128)) for stat in stats
        ]
        totals = [jnp.broadcast_to(stat[:, 64:65], (8, 128)) for stat in stats]
        top = tops[0]
        for t in tops[1:]:
            top = jnp.maximum(top, t)
        high = top.astype(BF16).astype(F32)
        low = (top - high).astype(BF16).astype(F32)
        total = jnp.zeros((8, 128), F32)
        result = jnp.zeros((8, 128), F32)
        for t, s, part in zip(tops, totals, parts):
            factor = jnp.exp(t - (high + low))
            total += s * factor
            result += part[0:8] * factor
        return high, low, total, result

    loads[7].wait()
    loads[8].wait()
    position = lax.broadcasted_iota(jnp.int32, (8, 256), 1) + seq * 256
    each = range(16)
    scores = [
        lax.dot_general(agq[r], kc[r], (((1,), (1,)), ((), ())), preferred_element_type=F32)
        * scale
        for r in each
    ]
    valid = [position < lengths[r] for r in each]
    scores = [jnp.where(valid[r], scores[r], masked_score) for r in each]
    tops = [jnp.max(scores[r], axis=1, keepdims=True) for r in each]
    highs = [top.astype(BF16).astype(F32) for top in tops]
    lows = [(top - high).astype(BF16).astype(F32) for top, high in zip(tops, highs)]
    weights = [
        jnp.where(valid[r], jnp.exp(scores[r] - (highs[r] + lows[r])), 0.0) for r in each
    ]
    totals = [jnp.sum(weights[r], axis=1, keepdims=True) for r in each]
    results = [
        jnp.dot(weights[r].astype(BF16), vc[r], preferred_element_type=F32) for r in each
    ]
    for r in each:
        rso_src[r] = packed(highs[r], lows[r], totals[r], results[r])
    @pl.when(core == 0)
    def _():
        for k, (dy, dz) in enumerate(WINDOW):
            send(7, rso_src.at[row_of(dy, dz)], rso.at[k], (dy, dz, 1))
        send(7, rso_src.at[first], rso.at[15], (0, 0, 1))
        bundle(13, ago).wait_recv()

    @pl.when(core == 1)
    def _():
        for k, (dy, dz) in enumerate(WINDOW):
            send(14, rso_src.at[row_of(dy, dz)], rso.at[k + 16], (dy, dz, 0))

        bundle(7, rso.at[0:16]).wait_recv()
        z2o[0, 0] = packed(*merged([rso[k] for k in range(16)]))
        bundle(14, rso.at[16:31]).wait_recv()
        z2o[0, 1] = packed(*merged([rso_src[first]] + [rso[k] for k in range(16, 31)]))
        for k, dz in enumerate(QUARTER):
            send(8, z2o.at[0], z2o.at[k + 1], (0, dz, 0))

        def attended(slot, own_score, value_own):
            high, low, total, result = merged([z2o[k, slot] for k in range(1, 5)])
            top = high + low
            peak = jnp.maximum(top, own_score)
            factor = jnp.exp(top - peak)
            own_weight = jnp.exp(own_score - peak)
            summed = result * factor + own_weight * value_own
            return (summed / (total * factor + own_weight)).astype(BF16)

        bundle(8, z2o.at[1:5]).wait_recv()
        ago_src[...] = attended(0, own[0, 0:8, :], own[0, 8:16, :])
        ago[mine] = attended(1, own[1, 0:8, :], own[1, 8:16, :])
        for dy, dz in WINDOW:
            send(13, ago_src, ago.at[mine], (dy, dz, -1))
            send(9, ago.at[mine], ago.at[mine], (dy, dz, 0))
        send(13, ago_src, ago.at[mine], (0, 0, -1))
        bundle(9, ago.at[0:15]).wait_recv()

    loads[9].wait()
    flat[0:128, :] = ago[...].astype(F32).reshape(128, 128)
    projected = jnp.zeros((16, 128), F32)
    for j in range(8):
        projected += jnp.dot(
            flat[pl.ds(j, 16, stride=8), :].astype(BF16),
            wo[j * 128 : (j + 1) * 128, :],
            preferred_element_type=F32,
        )
    hbuf[0] = projected.astype(BF16)
    for k, dh in enumerate(HEADS):
        send(10, hbuf.at[0], hbuf.at[k + 1], (0, 0, dh))
    bundle(10, hbuf.at[1:8]).wait_recv()
    out[...] = jnp.sum(hbuf[...].astype(F32), axis=0).astype(BF16)

    sent = [
        (0, t1a.at[0:15]), (2, rsb), (3, z2b.at[1:5]), (4, ups), (10, hbuf.at[1:8]),
    ]
    for stage, view in sent:
        bundle(stage, view).wait_send()

    @pl.when(core == 0)
    def _():
        bundle(17, t1_src).wait_send()
        bundle(12, own_in).wait_send()
        bundle(15, ups_in.at[0:4]).wait_send()
        bundle(7, rso.at[0:16]).wait_send()

    @pl.when(core == 1)
    def _():
        bundle(1, t1b.at[1:16]).wait_send()
        bundle(11, ups_in.at[4:7]).wait_send()
        bundle(5, z2e.at[1:5]).wait_send()
        bundle(16, agq).wait_send()
        bundle(6, agq.at[0:15]).wait_send()
        bundle(14, rso.at[16:31]).wait_send()
        bundle(8, z2o.at[1:5]).wait_send()
        bundle(13, ago).wait_send()
        bundle(9, ago.at[0:15]).wait_send()


def body(hid, gain, wq, wk, wv, wo, down, up, choice, lengths, kc, vc):
    anywhere = pl.BlockSpec(memory_space=pl.ANY)
    return pl.pallas_call(
        kernel,
        out_shape=pltpu.VMEM((16, 128), BF16),
        in_specs=[anywhere] * 12,
        out_specs=pl.BlockSpec(memory_space=pltpu.VMEM),
        scratch_shapes=[
            pltpu.VMEM((16, 128), BF16),
            pltpu.VMEM((1, 128), BF16),
            pltpu.VMEM((128, 1024), BF16),
            pltpu.VMEM((128, 128), BF16),
            pltpu.VMEM((128, 128), BF16),
            pltpu.VMEM((1024, 128), BF16),
            pltpu.VMEM((1024, 128), BF16),
            pltpu.VMEM((8, 16, 1024), BF16),
            pltpu.VMEM((16, 256, 128), BF16),
            pltpu.VMEM((16, 256, 128), BF16),
            pltpu.SMEM((16,), jnp.int32),
            pltpu.SMEM((16,), jnp.int32),
            pltpu.VMEM((2, 128), F32),
            pltpu.VMEM((32, 2, 128), F32),
            pltpu.VMEM((16, 2, 128), F32),
            pltpu.VMEM((256, 128), F32),
            pltpu.VMEM((16, 16, 128), BF16),
            pltpu.VMEM((15, 16, 128), BF16),
            pltpu.VMEM((5, 16, 128), BF16),
            pltpu.VMEM((4, 4, 16, 1024), BF16),
            pltpu.VMEM((3, 4, 16, 1024), BF16),
            pltpu.VMEM((4, 16, 1024), BF16),
            pltpu.VMEM((7, 16, 1024), BF16),
            pltpu.VMEM((5, 2, 8, 128), BF16),
            pltpu.VMEM((8, 128), BF16),
            pltpu.VMEM((16, 8, 128), BF16),
            pltpu.VMEM((16, 16, 128), BF16),
            pltpu.VMEM((31, 16, 128), BF16),
            pltpu.VMEM((5, 2, 16, 128), BF16),
            pltpu.VMEM((16, 128), F32),
            pltpu.VMEM((16, 128), F32),
            pltpu.VMEM((2, 16, 128), F32),
            pltpu.VMEM((8, 128), BF16),
            pltpu.VMEM((16, 8, 128), BF16),
            pltpu.VMEM((8, 16, 128), BF16),
            pltpu.SemaphoreType.DMA((12,)),
            pltpu.SemaphoreType.DMA((STAGES,)),
            pltpu.SemaphoreType.DMA((STAGES,)),
            pltpu.SemaphoreType.REGULAR,
        ],
        compiler_params=pltpu.CompilerParams(collective_id=0, has_side_effects=True),
    )(
        hid, gain.reshape(1, 128), wq, wk, wv, wo, down.reshape(1024, 128), up,
        choice, lengths, kc.reshape(16, 256, 128), vc.reshape(16, 256, 128),
    )


def solution(mesh):
    placed = (
        P(None, "seq"),
        P("seq"),
        P("seq", "head"),
        P("seq", "head"),
        P("seq", "head"),
        P("head", "seq"),
        P("head", None, "seq"),
        P("seq", None, "head"),
        P(),
        P(),
        P(None, "seq", "head", None),
        P(None, "seq", "head", None),
    )
    return jax.shard_map(
        body, mesh=mesh, in_specs=placed, out_specs=P(None, "seq"), check_vma=False
    )
```
